8 devices in a mesh: dp: 2 (over z, y), cp: 4 (over x, core).
Axes of the slice: x: 2, y: 2, z: 1, core: 2. Of those that a mesh axis runs over, the one named last changes fastest.
Arguments:
- x: bfloat16 [512, 2048], P(('dp', 'cp')), parts along dimension 0
- k_cache: bfloat16 [32768, 4, 128], P(('dp', 'cp')), parts along dimension 0
- v_cache: bfloat16 [32768, 4, 128], P(('dp', 'cp')), parts along dimension 0
- ln_gain: bfloat16 [2048], replicated
- w_q: bfloat16 [2048, 4096], replicated
- w_k: bfloat16 [2048, 512], replicated
- w_v: bfloat16 [2048, 512], replicated
- w_o: bfloat16 [4096, 2048], replicated
- q_gain: bfloat16 [128], replicated
- k_gain: bfloat16 [128], replicated
Outputs:
- output 1: bfloat16 [512, 2048], P(('dp', 'cp')), parts along dimension 0
- output 2: bfloat16 [512, 4, 128], P(('dp', 'cp')), parts along dimension 0
- output 3: bfloat16 [512, 4, 128], P(('dp', 'cp')), parts along dimension 0
There are 2 independent parts. The reference program is written for one: setup_inputs(seed, part) draws one part's arguments, and reference() takes and returns one part's arrays. A program takes and returns all parts, laid end to end along the dimension named above; an argument that names none is the same for every part.
All inputs are finite; a program needn't handle non-finite values.
Results may differ from the reference program's by a relative error of at most 0.0107701.
Values are sent between devices in bfloat16 or wider.
A program may use at most 1 GiB of HBM per device.

```python
import jax
import jax.numpy as jnp
from jax import lax

HIDDEN = 2048
Q_HEADS = 32
KV_HEADS = 4
HEAD_DIM = 128
NEW_LEN = 256
PREFIX_LEN = 16384
ROW_BLOCK = 16
ROPE_THETA = 1.0e6
NORM_EPS = 1.0e-6


def setup_inputs(seed: int = 0, part: int = 0) -> dict:
    part_key = jax.random.fold_in(jax.random.key(seed), part)
    part_keys = jax.random.split(part_key, 3)
    shared = jax.random.split(jax.random.key(seed + 1), 7)
    q_width = Q_HEADS * HEAD_DIM
    kv_width = KV_HEADS * HEAD_DIM
    total_len = PREFIX_LEN + NEW_LEN
    x = jax.random.normal(part_keys[0], (NEW_LEN, HIDDEN), jnp.float32)
    k_cache = jax.random.normal(part_keys[1], (PREFIX_LEN, KV_HEADS, HEAD_DIM), jnp.float32)
    v_cache = jax.random.normal(part_keys[2], (PREFIX_LEN, KV_HEADS, HEAD_DIM), jnp.float32)
    ln_gain = 1.0 + 0.4 * jax.random.normal(shared[0], (HIDDEN,), jnp.float32)
    w_q = jax.random.normal(shared[1], (HIDDEN, q_width), jnp.float32) * HIDDEN ** -0.5
    w_k = jax.random.normal(shared[2], (HIDDEN, kv_width), jnp.float32) * HIDDEN ** -0.5
    w_v = jax.random.normal(shared[3], (HIDDEN, kv_width), jnp.float32) * HIDDEN ** -0.5
    w_o = jax.random.normal(shared[4], (q_width, HIDDEN), jnp.float32) * (0.5 * (total_len / q_width) ** 0.5)
    q_gain = 1.0 + 0.3 * jax.random.normal(shared[5], (HEAD_DIM,), jnp.float32)
    k_gain = 1.5 + 0.3 * jax.random.normal(shared[6], (HEAD_DIM,), jnp.float32)
    return {'x': x.astype(jnp.bfloat16), 'k_cache': k_cache.astype(jnp.bfloat16), 'v_cache': v_cache.astype(jnp.bfloat16), 'ln_gain': ln_gain.astype(jnp.bfloat16), 'w_q': w_q.astype(jnp.bfloat16), 'w_k': w_k.astype(jnp.bfloat16), 'w_v': w_v.astype(jnp.bfloat16), 'w_o': w_o.astype(jnp.bfloat16), 'q_gain': q_gain.astype(jnp.bfloat16), 'k_gain': k_gain.astype(jnp.bfloat16)}


def rms_norm(vals, gain):
    mean_sq = jnp.mean(vals * vals, axis=-1, keepdims=True)
    return vals * lax.rsqrt(mean_sq + NORM_EPS) * gain


def apply_rope(vals, positions):
    half = HEAD_DIM // 2
    inv_freq = ROPE_THETA ** (-jnp.arange(half, dtype=jnp.float32) * (2.0 / HEAD_DIM))
    angles = positions.astype(jnp.float32)[:, None] * inv_freq[None, :]
    cos_tab = jnp.cos(angles)[:, None, :]
    sin_tab = jnp.sin(angles)[:, None, :]
    first = vals[..., :half]
    second = vals[..., half:]
    return jnp.concatenate([first * cos_tab - second * sin_tab, second * cos_tab + first * sin_tab], axis=-1)


def reference(x, k_cache, v_cache, ln_gain, w_q, w_k, w_v, w_o, q_gain, k_gain):
    group = Q_HEADS // KV_HEADS
    scale = HEAD_DIM ** -0.5
    x_wide = x.astype(jnp.float32)
    hidden = rms_norm(x_wide, ln_gain.astype(jnp.float32)).astype(jnp.bfloat16)
    q_raw = jnp.dot(hidden, w_q, preferred_element_type=jnp.float32).astype(jnp.bfloat16)
    k_raw = jnp.dot(hidden, w_k, preferred_element_type=jnp.float32).astype(jnp.bfloat16)
    v_new = jnp.dot(hidden, w_v, preferred_element_type=jnp.float32).astype(jnp.bfloat16).reshape(NEW_LEN, KV_HEADS, HEAD_DIM)
    positions = PREFIX_LEN + jnp.arange(NEW_LEN)
    q_rot = apply_rope(rms_norm(q_raw.reshape(NEW_LEN, Q_HEADS, HEAD_DIM).astype(jnp.float32), q_gain.astype(jnp.float32)), positions).astype(jnp.bfloat16)
    k_new = apply_rope(rms_norm(k_raw.reshape(NEW_LEN, KV_HEADS, HEAD_DIM).astype(jnp.float32), k_gain.astype(jnp.float32)), positions).astype(jnp.bfloat16)
    keys_all = jnp.concatenate([k_cache, k_new], axis=0).astype(jnp.float32)
    values_all = jnp.concatenate([v_cache, v_new], axis=0).astype(jnp.float32)
    key_pos = jnp.arange(PREFIX_LEN + NEW_LEN)
    block_count = NEW_LEN // ROW_BLOCK
    q_blocks = q_rot.reshape(block_count, ROW_BLOCK, KV_HEADS, group, HEAD_DIM)

    def block_attend(block):
        q_block, block_index = block
        row_pos = PREFIX_LEN + block_index * ROW_BLOCK + jnp.arange(ROW_BLOCK)
        scores = jnp.einsum('rkgd,skd->rkgs', q_block.astype(jnp.float32), keys_all) * scale
        allowed = key_pos[None, :] <= row_pos[:, None]
        scores = jnp.where(allowed[:, None, None, :], scores, -jnp.inf)
        peak = jnp.max(scores, axis=-1, keepdims=True)
        weights = jnp.exp(scores - peak)
        probs = weights / jnp.sum(weights, axis=-1, keepdims=True)
        return jnp.einsum('rkgs,skd->rkgd', probs, values_all)

    attended = lax.map(block_attend, (q_blocks, jnp.arange(block_count)))
    attended = attended.reshape(NEW_LEN, Q_HEADS * HEAD_DIM).astype(jnp.bfloat16)
    out = (x_wide + jnp.dot(attended, w_o, preferred_element_type=jnp.float32)).astype(jnp.bfloat16)
    return (out, k_new, v_new)
```

```python
import functools

import jax
import jax.numpy as jnp
import numpy as np
from jax import lax
from jax.experimental import pallas as pl
from jax.experimental.pallas import tpu as pltpu
from jax.sharding import PartitionSpec as P

HEAD_DIM = 128
HALF = HEAD_DIM // 2
ROPE_THETA = 1.0e6
NORM_EPS = 1.0e-6
LOG2E = 1.4426950408889634
SCALE2 = HEAD_DIM ** -0.5 * LOG2E
MESH = pl.DeviceIdType.MESH
F32 = jnp.float32
BF16 = jnp.bfloat16
ROWS = 64
CP = 4
KEYS = 4096
ALL_KEYS = KEYS + ROWS
KV = 4
GROUPS = 8
COLS = 256
TILE = 256
MSG = HEAD_DIM + 8
HIDDEN = 2048
CHUNK = 256


def rope_tables(prefix_len):
    freq = (ROPE_THETA ** (-np.arange(HALF, dtype=np.float64) * (2.0 / HEAD_DIM))).astype(np.float32)
    pos = (prefix_len + np.arange(CP * ROWS)).astype(np.float32).reshape(CP, 1, ROWS)
    angles = (pos * freq[None, :, None]).astype(np.float32)
    angles = np.concatenate([angles, angles], axis=2).astype(np.float64)
    return np.cos(angles).astype(np.float32), np.sin(angles).astype(np.float32)


def kernel(x_hbm, k_hbm, v_hbm, ln_ref, wq_hbm, wk_hbm, wv_hbm, wo_hbm, qg_ref, kg_ref, cos_ref, sin_ref,
           out_ref, knew_ref, vnew_ref,
           xall, hbuf, wbuf, wk, wv, kst, vst, kf, vf, ks, vt, qt, gq, gk, s_a, s_b, m_a, m_b,
           abuf, bbuf, rbuf, cbuf, obuf,
           x_sem, xs_sem, xr_sem, w_sem, kv_sem, cache_sem, wo_sem, as_sem, ar_sem, cs_sem, cr_sem):
    me = lax.axis_index("cp")
    dp = lax.axis_index("dp")
    partner = me + 1 - 2 * lax.rem(me, 2)
    cross = lax.rem(me + 2, CP)
    far = lax.rem(partner + 2, CP)

    def remote(src, dst, ssem, rsem, to):
        return pltpu.make_async_remote_copy(src_ref=src, dst_ref=dst, send_sem=ssem, recv_sem=rsem,
                                            device_id=(dp, to), device_id_type=MESH)

    x_copy = pltpu.make_async_copy(x_hbm, xall.at[0], x_sem)
    x_copy.start()
    wk_copy = pltpu.make_async_copy(wk_hbm, wk, kv_sem.at[0])
    wv_copy = pltpu.make_async_copy(wv_hbm, wv, kv_sem.at[1])

    def wq_copy(g):
        return pltpu.make_async_copy(wq_hbm.at[:, pl.ds(pl.multiple_of(g * 512, 512), 512)], wbuf.at[g], w_sem.at[g])

    def wo_copy(b):
        nb = b // 2
        kh = b % 2
        return pltpu.make_async_copy(wo_hbm.at[pl.ds(kh * 2048, 2048), pl.ds(nb * 512, 512)], wbuf.at[b], wo_sem.at[b])

    NC = 4
    CB = KEYS // NC

    def cache_copy(src, dst, j, n):
        return pltpu.make_async_copy(src.at[pl.ds(j * CB, CB)], dst.at[pl.ds(j * CB, CB)], cache_sem.at[n, j])

    for g in range(4):
        wq_copy(g).start()
    wk_copy.start()
    wv_copy.start()
    for g in range(4, GROUPS):
        wq_copy(g).start()
    for j in range(NC):
        cache_copy(k_hbm, kst, j, 0).start()
        cache_copy(v_hbm, vst, j, 1).start()

    barrier = pltpu.get_barrier_semaphore()
    for to in (partner, cross):
        pl.semaphore_signal(barrier, inc=1, device_id=(dp, to), device_id_type=MESH)
    pl.semaphore_wait(barrier, 2)
    x_copy.wait()
    x_to_cross = remote(xall.at[0], xall.at[2], xs_sem.at[1], xr_sem.at[1], cross)
    x_to_cross.start()
    x_to_partner = remote(xall.at[0], xall.at[1], xs_sem.at[0], xr_sem.at[0], partner)
    x_to_partner.start()
    x_forward = remote(xall.at[2], xall.at[3], xs_sem.at[2], xr_sem.at[2], partner)

    gq[...] = jnp.broadcast_to(qg_ref[...].astype(F32), (HEAD_DIM, HEAD_DIM)).T
    gk[...] = jnp.broadcast_to(kg_ref[...].astype(F32), (HEAD_DIM, HEAD_DIM)).T
    ln_gain = ln_ref[...].astype(F32)

    def normalise(slot):
        wide = xall[slot].astype(F32)
        mean_sq = jnp.mean(wide * wide, axis=-1, keepdims=True)
        hbuf[slot * ROWS:(slot + 1) * ROWS, :] = (wide * lax.rsqrt(mean_sq + NORM_EPS) * ln_gain).astype(BF16)

    def norm_rope(raw_t, gain, cos, sin):
        z = raw_t.astype(F32)
        mean_sq = jnp.mean(z * z, axis=0, keepdims=True)
        y = z * lax.rsqrt(mean_sq + NORM_EPS) * gain
        first, second = y[:HALF], y[HALF:]
        return jnp.concatenate([first * cos - second * sin, second * cos + first * sin], axis=0).astype(BF16)

    def project(pair, g):
        if isinstance(pair, int) and pair == 0:
            ids, units = (me, partner), (16 + 2 * g + 1, 16 + 2 * g)
        else:
            ids, units = (cross, far), (2 * g + 1, 2 * g)
        raw = jnp.dot(hbuf[pair * 128:(pair + 1) * 128, :], wbuf[g], preferred_element_type=F32).astype(BF16)
        for n in range(2):
            cos, sin = cos_ref[ids[n]], sin_ref[ids[n]]
            part = raw[n * ROWS:(n + 1) * ROWS]
            for hh in range(2):
                two = jnp.concatenate([part[:, hh * 256:hh * 256 + 128], part[:, hh * 256 + 128:hh * 256 + 256]], axis=0)
                qt[units[n], :, hh * 128:(hh + 1) * 128] = norm_rope(two.T, gq[...], cos, sin)

    normalise(0)
    x_to_partner.wait_recv()
    normalise(1)

    def pair0(g, carry):
        wq_copy(g).wait()
        project(0, g)
        return carry

    lax.fori_loop(0, GROUPS, pair0, 0)

    wk_copy.wait()
    wv_copy.wait()
    k_raw = jnp.dot(hbuf[0:ROWS, :], wk[...], preferred_element_type=F32).astype(BF16)
    v_raw = jnp.dot(hbuf[0:ROWS, :], wv[...], preferred_element_type=F32).astype(BF16)
    for hh in range(2):
        two = jnp.concatenate([k_raw[:, hh * 256:hh * 256 + 128], k_raw[:, hh * 256 + 128:hh * 256 + 256]], axis=0)
        back = norm_rope(two.T, gk[...], cos_ref[me], sin_ref[me]).T
        for n in range(2):
            ks[2 * hh + n, KEYS:ALL_KEYS, :] = back[n * ROWS:(n + 1) * ROWS]
            knew_ref[:, 2 * hh + n, :] = back[n * ROWS:(n + 1) * ROWS]
    for h in range(KV):
        one = v_raw[:, h * 128:(h + 1) * 128]
        vt[h, :, KEYS:ALL_KEYS] = one.T
        vnew_ref[:, h, :] = one

    x_to_cross.wait_recv()
    x_forward.start()
    for j in range(NC):
        cache_copy(k_hbm, kst, j, 0).wait()
        cache_copy(v_hbm, vst, j, 1).wait()

        def relayout(i, carry, j=j):
            at = pl.ds(pl.multiple_of(j * CB + i * CHUNK, CHUNK), CHUNK)
            kf[...] = kst[at].astype(F32).reshape(CHUNK * KV, HEAD_DIM)
            vf[...] = vst[at].astype(F32).reshape(CHUNK * KV, HEAD_DIM)
            for h in range(KV):
                ks[h, at, :] = kf[pl.ds(h, CHUNK, stride=KV), :].astype(BF16)
                vt[h, :, at] = vf[pl.ds(h, CHUNK, stride=KV), :].astype(BF16).T
            return carry

        lax.fori_loop(0, CB // CHUNK, relayout, 0)

    normalise(2)
    x_forward.wait_recv()
    normalise(3)

    def pair1(g, carry):
        project(1, g)
        return carry

    lax.fori_loop(0, GROUPS, pair1, 0)
    for b in range(GROUPS):
        wo_copy(b).start()

    tiles = [(t * TILE, TILE) for t in range(KEYS // TILE)] + [(KEYS, ROWS)]

    def colmax(s, n):
        return jnp.max(s.reshape(n // 8, 8, COLS), axis=0)

    class Unit:
        pass

    def begin(u, s_ref, m_ref, dest):
        z = Unit()
        z.s, z.m = s_ref, m_ref
        z.peak = m_ref[0:1]
        z.head = lax.rem(u // 2, GROUPS) // 2
        z.acc = z.sum = None
        return z

    def begin_next(z, u, s_ref, m_ref, dest):
        z.s, z.m = s_ref, m_ref
        z.next_head = lax.rem(u // 2, GROUPS) // 2
        z.q = qt[u]
        z.dest = dest
        z.top = None
        return z

    def weigh(z, t):
        lo, n = tiles[t]
        p = jnp.exp2(z.s[lo:lo + n, :] * SCALE2 - z.peak)
        part = jnp.sum(p.reshape(n // 8, 8, COLS), axis=0)
        z.sum = part if z.sum is None else z.sum + part
        a = jnp.dot(vt[z.head, :, lo:lo + n], p.astype(BF16), preferred_element_type=F32)
        z.acc = a if z.acc is None else z.acc + a

    def score(z, t):
        lo, n = tiles[t]
        s = jnp.dot(ks[z.next_head, lo:lo + n, :], z.q, preferred_element_type=F32)
        if t == len(tiles) - 1:
            key = me * ROWS + lax.broadcasted_iota(jnp.int32, (n, COLS), 0)
            row = z.dest * ROWS + (lax.broadcasted_iota(jnp.int32, (n, COLS), 1) & (ROWS - 1))
            s = jnp.where(key <= row, s, -jnp.inf)
        z.s[lo:lo + n, :] = s
        top = colmax(s, n)
        z.top = top if z.top is None else jnp.maximum(z.top, top)

    def end_next(z):
        z.m[0:1] = jnp.max(z.top, axis=0, keepdims=True) * SCALE2

    def finish(z, ref, slot):
        ref[slot, 0:HEAD_DIM, :] = z.acc
        ref[slot, HEAD_DIM:HEAD_DIM + 1, :] = z.peak
        ref[slot, HEAD_DIM + 1:HEAD_DIM + 2, :] = jnp.sum(z.sum, axis=0, keepdims=True)

    def dests(i):
        return jnp.where(i < GROUPS, far, partner), jnp.where(i < GROUPS, cross, me)

    za, zb = Unit(), Unit()
    da, db = far, cross
    begin_next(za, 0, s_a, m_a, da)
    begin_next(zb, 1, s_b, m_b, db)
    for t in range(len(tiles)):
        score(za, t)
        score(zb, t)
    end_next(za)
    end_next(zb)

    def to_partner(i):
        return remote(abuf.at[i], rbuf.at[i], as_sem.at[i], ar_sem.at[i], partner)

    def to_cross(g):
        return remote(bbuf.at[g], cbuf.at[g], cs_sem.at[g], cr_sem.at[g], cross)

    def combine_cross(g):
        to_partner(g).wait_recv()
        m1, m2 = bbuf[g, 128:129, :], rbuf[g, 128:129, :]
        m = jnp.maximum(m1, m2)
        w1, w2 = jnp.exp2(m1 - m), jnp.exp2(m2 - m)
        bbuf[g, 0:128, :] = bbuf[g, 0:128, :] * w1 + rbuf[g, 0:128, :] * w2
        total = bbuf[g, 129:130, :] * w1 + rbuf[g, 129:130, :] * w2
        bbuf[g, 128:129, :] = m
        bbuf[g, 129:130, :] = total
        to_cross(g).start()

    def attend(i, last):
        a = begin(2 * i, s_a, m_a, None)
        b = begin(2 * i + 1, s_b, m_b, None)
        if not last:
            da, db = dests(i + 1)
            begin_next(a, 2 * i + 2, s_a, m_a, da)
            begin_next(b, 2 * i + 3, s_b, m_b, db)
        for t in range(len(tiles)):
            for z in (a, b):
                weigh(z, t)
                if not last:
                    score(z, t)
        finish(a, abuf, i)
        finish(b, bbuf, i)
        if not last:
            end_next(a)
            end_next(b)
        to_partner(i).start()

    def body(i, carry):
        @pl.when(jnp.logical_and(i >= 2, i < GROUPS + 2))
        def _():
            combine_cross(i - 2)

        attend(i, False)
        return carry

    lax.fori_loop(0, 2 * GROUPS - 1, body, 0)
    attend(2 * GROUPS - 1, True)

    for g in range(GROUPS):
        to_partner(GROUPS + g).wait_recv()
        to_cross(g).wait_recv()
        parts = ((bbuf, GROUPS + g), (rbuf, GROUPS + g), (cbuf, g))
        peaks = [ref[n, 128:129, :] for ref, n in parts]
        m = jnp.maximum(jnp.maximum(peaks[0], peaks[1]), peaks[2])
        ws = [jnp.exp2(p - m) for p in peaks]
        total = sum(ref[n, 129:130, :] * w for (ref, n), w in zip(parts, ws))
        inv = 1.0 / total
        o = sum(ref[n, 0:128, :] * (w * inv) for (ref, n), w in zip(parts, ws)).astype(BF16)
        for hh in range(2):
            rows = o[:, hh * 128:(hh + 1) * 128].T
            for n in range(2):
                col = (4 * g + 2 * hh + n) * HEAD_DIM
                obuf[:, col:col + HEAD_DIM] = rows[n * ROWS:(n + 1) * ROWS]

    for b in range(GROUPS):
        wo_copy(b).wait()
    for nb in range(4):
        cols = slice(nb * 512, (nb + 1) * 512)
        acc = jnp.dot(obuf[:, 0:2048], wbuf[2 * nb], preferred_element_type=F32)
        acc = acc + jnp.dot(obuf[:, 2048:4096], wbuf[2 * nb + 1], preferred_element_type=F32)
        out_ref[:, cols] = (xall[0, :, cols].astype(F32) + acc).astype(BF16)

    x_to_partner.wait_send()
    x_to_cross.wait_send()
    x_forward.wait_send()

    def drain(i, carry):
        to_partner(i).wait_send()
        return carry

    lax.fori_loop(0, 2 * GROUPS, drain, 0)

    def drain_cross(g, carry):
        to_cross(g).wait_send()
        return carry

    lax.fori_loop(0, GROUPS, drain_cross, 0)


def solution(mesh):
    row_spec = P(('dp', 'cp'), None)
    cache_spec = P(('dp', 'cp'), None, None)
    whole = P()
    any_spec = pl.BlockSpec(memory_space=pl.ANY)
    vmem_spec = pl.BlockSpec(memory_space=pltpu.VMEM)

    def device_step(x_rows, k_cache, v_cache, ln_gain, w_q, w_k, w_v, w_o, q_gain, k_gain):
        cos, sin = rope_tables(k_cache.shape[0] * CP)
        dma = pltpu.SemaphoreType.DMA
        return pl.pallas_call(
            kernel,
            out_shape=(jax.ShapeDtypeStruct((ROWS, HIDDEN), BF16),
                       jax.ShapeDtypeStruct((ROWS, KV, HEAD_DIM), BF16),
                       jax.ShapeDtypeStruct((ROWS, KV, HEAD_DIM), BF16)),
            in_specs=[any_spec, any_spec, any_spec, vmem_spec, any_spec, any_spec, any_spec, any_spec,
                      vmem_spec, vmem_spec, vmem_spec, vmem_spec],
            out_specs=(vmem_spec, vmem_spec, vmem_spec),
            scratch_shapes=[
                pltpu.VMEM((4, ROWS, HIDDEN), BF16),
                pltpu.VMEM((4 * ROWS, HIDDEN), BF16),
                pltpu.VMEM((GROUPS, 2048, 512), BF16),
                pltpu.VMEM((HIDDEN, 512), BF16),
                pltpu.VMEM((HIDDEN, 512), BF16),
                pltpu.VMEM((KEYS, KV, HEAD_DIM), BF16),
                pltpu.VMEM((KEYS, KV, HEAD_DIM), BF16),
                pltpu.VMEM((CHUNK * KV, HEAD_DIM), F32),
                pltpu.VMEM((CHUNK * KV, HEAD_DIM), F32),
                pltpu.VMEM((KV, ALL_KEYS, HEAD_DIM), BF16),
                pltpu.VMEM((KV, HEAD_DIM, ALL_KEYS), BF16),
                pltpu.VMEM((4 * GROUPS, HEAD_DIM, COLS), BF16),
                pltpu.VMEM((HEAD_DIM, HEAD_DIM), F32),
                pltpu.VMEM((HEAD_DIM, HEAD_DIM), F32),
                pltpu.VMEM((ALL_KEYS, COLS), F32),
                pltpu.VMEM((ALL_KEYS, COLS), F32),
                pltpu.VMEM((8, COLS), F32),
                pltpu.VMEM((8, COLS), F32),
                pltpu.VMEM((2 * GROUPS, MSG, COLS), F32),
                pltpu.VMEM((2 * GROUPS, MSG, COLS), F32),
                pltpu.VMEM((2 * GROUPS, MSG, COLS), F32),
                pltpu.VMEM((GROUPS, MSG, COLS), F32),
                pltpu.VMEM((ROWS, 4096), BF16),
                dma, dma((3,)), dma((3,)), dma((GROUPS,)), dma((2,)), dma((2, 4)), dma((GROUPS,)),
                dma((2 * GROUPS,)), dma((2 * GROUPS,)), dma((GROUPS,)), dma((GROUPS,)),
            ],
            compiler_params=pltpu.CompilerParams(collective_id=0, has_side_effects=True,
                                                 vmem_limit_bytes=67043328),
        )(x_rows, k_cache, v_cache, ln_gain.reshape(1, -1), w_q, w_k, w_v, w_o,
          q_gain.reshape(1, -1), k_gain.reshape(1, -1), jnp.asarray(cos), jnp.asarray(sin))

    return jax.shard_map(device_step, mesh=mesh,
                         in_specs=(row_spec, cache_spec, cache_spec, whole, whole, whole, whole, whole, whole, whole),
                         out_specs=(row_spec, cache_spec, cache_spec), check_vma=False)
```

```python
import functools

import jax
import jax.numpy as jnp
import numpy as np
from jax import lax
from jax.experimental import pallas as pl
from jax.experimental.pallas import tpu as pltpu
from jax.sharding import PartitionSpec as P

HEAD_DIM = 128
HALF = HEAD_DIM // 2
ROPE_THETA = 1.0e6
NORM_EPS = 1.0e-6
LOG2E = 1.4426950408889634
SCALE2 = HEAD_DIM ** -0.5 * LOG2E
MESH = pl.DeviceIdType.MESH
F32 = jnp.float32
BF16 = jnp.bfloat16
ROWS = 64
CP = 4
KEYS = 4096
ALL_KEYS = KEYS + ROWS
KV = 4
GROUPS = 8
COLS = 256
TILE = 256
MSG = HEAD_DIM + 8
HIDDEN = 2048
CHUNK = 512


def rope_tables(prefix_len):
    freq = (ROPE_THETA ** (-np.arange(HALF, dtype=np.float64) * (2.0 / HEAD_DIM))).astype(np.float32)
    pos = (prefix_len + np.arange(CP * ROWS)).astype(np.float32).reshape(CP, 1, ROWS)
    angles = (pos * freq[None, :, None]).astype(np.float32)
    angles = np.concatenate([angles, angles], axis=2).astype(np.float64)
    return np.cos(angles).astype(np.float32), np.sin(angles).astype(np.float32)


def kernel(x_hbm, k_hbm, v_hbm, ln_ref, wq_hbm, wk_hbm, wv_hbm, wo_hbm, qg_ref, kg_ref, cos_hbm, sin_hbm,
           out_ref, knew_ref, vnew_ref,
           cos_ref, sin_ref, xall, hbuf, wbuf, wk, wv, kst, vst, kf, vf, ks, vt, qt, gq, gk, s_a, s_b, m_a, m_b,
           abuf, bbuf, rbuf, cbuf, obuf,
           x_sem, xs_sem, xr_sem, w_sem, kv_sem, tab_sem, cache_sem, wo_sem, as_sem, ar_sem, cs_sem, cr_sem):
    me = lax.axis_index("cp")
    dp = lax.axis_index("dp")
    partner = me + 1 - 2 * lax.rem(me, 2)
    cross = lax.rem(me + 2, CP)
    far = lax.rem(partner + 2, CP)

    def remote(src, dst, ssem, rsem, to):
        return pltpu.make_async_remote_copy(src_ref=src, dst_ref=dst, send_sem=ssem, recv_sem=rsem,
                                            device_id=(dp, to), device_id_type=MESH)

    x_copy = pltpu.make_async_copy(x_hbm, xall.at[0], x_sem)
    x_copy.start()
    wk_copy = pltpu.make_async_copy(wk_hbm, wk, kv_sem.at[0])
    wv_copy = pltpu.make_async_copy(wv_hbm, wv, kv_sem.at[1])

    def wq_copy(g):
        return pltpu.make_async_copy(wq_hbm.at[:, pl.ds(pl.multiple_of(g * 512, 512), 512)], wbuf.at[g], w_sem.at[g])

    def wo_copy(b):
        nb = b // 2
        kh = b % 2
        return pltpu.make_async_copy(wo_hbm.at[pl.ds(kh * 2048, 2048), pl.ds(nb * 512, 512)], wbuf.at[b], wo_sem.at[b])

    CB = KEYS // GROUPS

    def cache_copy(src, dst, j, n):
        return pltpu.make_async_copy(src.at[pl.ds(j * CB, CB)], dst.at[pl.ds(j * CB, CB)], cache_sem.at[n, j])

    cos_copy = pltpu.make_async_copy(cos_hbm, cos_ref, tab_sem.at[0])
    sin_copy = pltpu.make_async_copy(sin_hbm, sin_ref, tab_sem.at[1])
    cos_copy.start()
    sin_copy.start()
    for g in range(GROUPS):
        wq_copy(g).start()
        cache_copy(k_hbm, kst, g, 0).start()
        cache_copy(v_hbm, vst, g, 1).start()
    wk_copy.start()
    wv_copy.start()

    barrier = pltpu.get_barrier_semaphore()
    for to in (partner, cross):
        pl.semaphore_signal(barrier, inc=1, device_id=(dp, to), device_id_type=MESH)
    pl.semaphore_wait(barrier, 2)
    x_copy.wait()
    x_to_cross = remote(xall.at[0], xall.at[2], xs_sem.at[1], xr_sem.at[1], cross)
    x_to_cross.start()
    x_to_partner = remote(xall.at[0], xall.at[1], xs_sem.at[0], xr_sem.at[0], partner)
    x_to_partner.start()
    x_forward = remote(xall.at[2], xall.at[3], xs_sem.at[2], xr_sem.at[2], partner)

    gq[...] = jnp.broadcast_to(qg_ref[...].astype(F32), (HEAD_DIM, HEAD_DIM)).T
    gk[...] = jnp.broadcast_to(kg_ref[...].astype(F32), (HEAD_DIM, HEAD_DIM)).T
    ln_gain = ln_ref[...].astype(F32).reshape(1, HIDDEN)

    def normalise(slot):
        wide = xall[slot].astype(F32)
        mean_sq = jnp.mean(wide * wide, axis=-1, keepdims=True)
        hbuf[slot * ROWS:(slot + 1) * ROWS, :] = (wide * lax.rsqrt(mean_sq + NORM_EPS) * ln_gain).astype(BF16)

    def norm_rope(raw_t, gain, cos, sin):
        z = raw_t.astype(F32)
        mean_sq = jnp.mean(z * z, axis=0, keepdims=True)
        y = z * lax.rsqrt(mean_sq + NORM_EPS) * gain
        first, second = y[:HALF], y[HALF:]
        return jnp.concatenate([first * cos - second * sin, second * cos + first * sin], axis=0).astype(BF16)

    def project(pair, g):
        if isinstance(pair, int) and pair == 0:
            ids, units = (me, partner), (16 + 2 * g + 1, 16 + 2 * g)
        else:
            ids, units = (cross, far), (2 * g + 1, 2 * g)
        raw = jnp.dot(hbuf[pair * 128:(pair + 1) * 128, :], wbuf[g], preferred_element_type=F32).astype(BF16)
        for n in range(2):
            cos, sin = cos_ref[ids[n]], sin_ref[ids[n]]
            part = raw[n * ROWS:(n + 1) * ROWS]
            for hh in range(2):
                two = jnp.concatenate([part[:, hh * 256:hh * 256 + 128], part[:, hh * 256 + 128:hh * 256 + 256]], axis=0)
                qt[units[n], :, hh * 128:(hh + 1) * 128] = norm_rope(two.T, gq[...], cos, sin)

    normalise(0)
    cos_copy.wait()
    sin_copy.wait()
    x_to_partner.wait_recv()
    normalise(1)

    def pair0(g, carry):
        wq_copy(g).wait()
        cache_copy(k_hbm, kst, g, 0).wait()
        cache_copy(v_hbm, vst, g, 1).wait()
        project(0, g)
        at = pl.ds(pl.multiple_of(g * CHUNK, CHUNK), CHUNK)
        kf[...] = kst[at].astype(F32).reshape(CHUNK * KV, HEAD_DIM)
        vf[...] = vst[at].astype(F32).reshape(CHUNK * KV, HEAD_DIM)
        for h in range(KV):
            ks[h, at, :] = kf[pl.ds(h, CHUNK, stride=KV), :].astype(BF16)
            vt[h, :, at] = vf[pl.ds(h, CHUNK, stride=KV), :].astype(BF16).T
        return carry

    lax.fori_loop(0, GROUPS, pair0, 0)
    x_to_cross.wait_recv()
    x_forward.start()

    wk_copy.wait()
    wv_copy.wait()
    k_raw = jnp.dot(hbuf[0:ROWS, :], wk[...], preferred_element_type=F32).astype(BF16)
    v_raw = jnp.dot(hbuf[0:ROWS, :], wv[...], preferred_element_type=F32).astype(BF16)
    for hh in range(2):
        two = jnp.concatenate([k_raw[:, hh * 256:hh * 256 + 128], k_raw[:, hh * 256 + 128:hh * 256 + 256]], axis=0)
        back = norm_rope(two.T, gk[...], cos_ref[me], sin_ref[me]).T
        for n in range(2):
            ks[2 * hh + n, KEYS:ALL_KEYS, :] = back[n * ROWS:(n + 1) * ROWS]
            knew_ref[:, 2 * hh + n, :] = back[n * ROWS:(n + 1) * ROWS]
    for h in range(KV):
        one = v_raw[:, h * 128:(h + 1) * 128]
        vt[h, :, KEYS:ALL_KEYS] = one.T
        vnew_ref[:, h, :] = one

    normalise(2)
    x_forward.wait_recv()
    normalise(3)

    project(1, 0)
    project(1, 1)

    tiles = [(t * TILE, TILE) for t in range(KEYS // TILE)] + [(KEYS, ROWS)]

    def colmax(s, n):
        return jnp.max(s.reshape(n // 8, 8, COLS), axis=0)

    class Unit:
        pass

    def begin(u, s_ref, m_ref, dest):
        z = Unit()
        z.s, z.m = s_ref, m_ref
        z.peak = m_ref[0:1]
        z.head = lax.rem(u // 2, GROUPS) // 2
        z.acc = z.sum = None
        return z

    def begin_next(z, u, s_ref, m_ref, dest):
        z.s, z.m = s_ref, m_ref
        z.next_head = lax.rem(u // 2, GROUPS) // 2
        z.q = qt[u]
        z.dest = dest
        z.top = None
        return z

    def weigh(z, t):
        lo, n = tiles[t]
        p = jnp.exp2(z.s[lo:lo + n, :] * SCALE2 - z.peak)
        part = jnp.sum(p.reshape(n // 8, 8, COLS), axis=0)
        z.sum = part if z.sum is None else z.sum + part
        a = jnp.dot(vt[z.head, :, lo:lo + n], p.astype(BF16), preferred_element_type=F32)
        z.acc = a if z.acc is None else z.acc + a

    def score(z, t):
        lo, n = tiles[t]
        s = jnp.dot(ks[z.next_head, lo:lo + n, :], z.q, preferred_element_type=F32)
        if t == len(tiles) - 1:
            key = me * ROWS + lax.broadcasted_iota(jnp.int32, (n, COLS), 0)
            row = z.dest * ROWS + (lax.broadcasted_iota(jnp.int32, (n, COLS), 1) & (ROWS - 1))
            s = jnp.where(key <= row, s, -jnp.inf)
        z.s[lo:lo + n, :] = s
        top = colmax(s, n)
        z.top = top if z.top is None else jnp.maximum(z.top, top)

    def end_next(z):
        z.m[0:1] = jnp.max(z.top, axis=0, keepdims=True) * SCALE2

    def finish(z, ref, slot):
        ref[slot, 0:HEAD_DIM, :] = z.acc
        ref[slot, HEAD_DIM:HEAD_DIM + 1, :] = z.peak
        ref[slot, HEAD_DIM + 1:HEAD_DIM + 2, :] = jnp.sum(z.sum, axis=0, keepdims=True)

    def dests(i):
        return jnp.where(i < GROUPS, far, partner), jnp.where(i < GROUPS, cross, me)

    za, zb = Unit(), Unit()
    da, db = far, cross
    begin_next(za, 0, s_a, m_a, da)
    begin_next(zb, 1, s_b, m_b, db)
    for t in range(len(tiles)):
        score(za, t)
        score(zb, t)
    end_next(za)
    end_next(zb)

    def to_partner(i):
        return remote(abuf.at[i], rbuf.at[i], as_sem.at[i], ar_sem.at[i], partner)

    def to_cross(g):
        return remote(bbuf.at[g], cbuf.at[g], cs_sem.at[g], cr_sem.at[g], cross)

    def combine_cross(g):
        to_partner(g).wait_recv()
        m1, m2 = bbuf[g, 128:129, :], rbuf[g, 128:129, :]
        m = jnp.maximum(m1, m2)
        w1, w2 = jnp.exp2(m1 - m), jnp.exp2(m2 - m)
        bbuf[g, 0:128, :] = bbuf[g, 0:128, :] * w1 + rbuf[g, 0:128, :] * w2
        total = bbuf[g, 129:130, :] * w1 + rbuf[g, 129:130, :] * w2
        bbuf[g, 128:129, :] = m
        bbuf[g, 129:130, :] = total
        to_cross(g).start()

    def attend(i, last, ahead=False):
        a = begin(2 * i, s_a, m_a, None)
        b = begin(2 * i + 1, s_b, m_b, None)
        if not last:
            da, db = dests(i + 1)
            begin_next(a, 2 * i + 2, s_a, m_a, da)
            begin_next(b, 2 * i + 3, s_b, m_b, db)
        for t in range(len(tiles)):
            for z in (a, b):
                weigh(z, t)
                if not last:
                    score(z, t)
            if ahead and t == 2:
                project(1, i + 2)
        finish(a, abuf, i)
        finish(b, bbuf, i)
        if not last:
            end_next(a)
            end_next(b)
        to_partner(i).start()

    def body(ahead, i, carry):
        @pl.when(jnp.logical_and(i >= 2, i < GROUPS + 2))
        def _():
            combine_cross(i - 2)

        attend(i, False, ahead)
        return carry

    lax.fori_loop(0, GROUPS - 2, functools.partial(body, True), 0)
    for b in range(GROUPS):
        wo_copy(b).start()
    lax.fori_loop(GROUPS - 2, 2 * GROUPS - 1, functools.partial(body, False), 0)
    attend(2 * GROUPS - 1, True)

    for g in range(GROUPS):
        to_partner(GROUPS + g).wait_recv()
        to_cross(g).wait_recv()
        parts = ((bbuf, GROUPS + g), (rbuf, GROUPS + g), (cbuf, g))
        peaks = [ref[n, 128:129, :] for ref, n in parts]
        m = jnp.maximum(jnp.maximum(peaks[0], peaks[1]), peaks[2])
        ws = [jnp.exp2(p - m) for p in peaks]
        total = sum(ref[n, 129:130, :] * w for (ref, n), w in zip(parts, ws))
        inv = 1.0 / total
        o = sum(ref[n, 0:128, :] * (w * inv) for (ref, n), w in zip(parts, ws)).astype(BF16)
        for hh in range(2):
            rows = o[:, hh * 128:(hh + 1) * 128].T
            for n in range(2):
                col = (4 * g + 2 * hh + n) * HEAD_DIM
                obuf[:, col:col + HEAD_DIM] = rows[n * ROWS:(n + 1) * ROWS]

    for b in range(GROUPS):
        wo_copy(b).wait()
    for nb in range(4):
        cols = slice(nb * 512, (nb + 1) * 512)
        acc = jnp.dot(obuf[:, 0:2048], wbuf[2 * nb], preferred_element_type=F32)
        acc = acc + jnp.dot(obuf[:, 2048:4096], wbuf[2 * nb + 1], preferred_element_type=F32)
        out_ref[:, cols] = (xall[0, :, cols].astype(F32) + acc).astype(BF16)

    x_to_partner.wait_send()
    x_to_cross.wait_send()
    x_forward.wait_send()

    def drain(i, carry):
        to_partner(i).wait_send()
        return carry

    lax.fori_loop(0, 2 * GROUPS, drain, 0)

    def drain_cross(g, carry):
        to_cross(g).wait_send()
        return carry

    lax.fori_loop(0, GROUPS, drain_cross, 0)


def hand_over(*refs):
    for src, dst in zip(refs[:3], refs[3:]):
        dst[...] = src[...]


def solution(mesh):
    row_spec = P(('dp', 'cp'), None)
    cache_spec = P(('dp', 'cp'), None, None)
    whole = P()
    any_spec = pl.BlockSpec(memory_space=pl.ANY)
    vmem_spec = pl.BlockSpec(memory_space=pltpu.VMEM)

    def device_step(x_rows, k_cache, v_cache, ln_gain, w_q, w_k, w_v, w_o, q_gain, k_gain):
        cos, sin = rope_tables(k_cache.shape[0] * CP)
        dma = pltpu.SemaphoreType.DMA
        results = pl.pallas_call(
            kernel,
            out_shape=(jax.ShapeDtypeStruct((ROWS, HIDDEN), BF16),
                       jax.ShapeDtypeStruct((ROWS, KV, HEAD_DIM), BF16),
                       jax.ShapeDtypeStruct((ROWS, KV, HEAD_DIM), BF16)),
            in_specs=[any_spec, any_spec, any_spec, vmem_spec, any_spec, any_spec, any_spec, any_spec,
                      vmem_spec, vmem_spec, any_spec, any_spec],
            out_specs=(vmem_spec, vmem_spec, vmem_spec),
            scratch_shapes=[
                pltpu.VMEM((CP, HALF, 128), F32),
                pltpu.VMEM((CP, HALF, 128), F32),
                pltpu.VMEM((4, ROWS, HIDDEN), BF16),
                pltpu.VMEM((4 * ROWS, HIDDEN), BF16),
                pltpu.VMEM((GROUPS, 2048, 512), BF16),
                pltpu.VMEM((HIDDEN, 512), BF16),
                pltpu.VMEM((HIDDEN, 512), BF16),
                pltpu.VMEM((KEYS, KV, HEAD_DIM), BF16),
                pltpu.VMEM((KEYS, KV, HEAD_DIM), BF16),
                pltpu.VMEM((CHUNK * KV, HEAD_DIM), F32),
                pltpu.VMEM((CHUNK * KV, HEAD_DIM), F32),
                pltpu.VMEM((KV, ALL_KEYS, HEAD_DIM), BF16),
                pltpu.VMEM((KV, HEAD_DIM, ALL_KEYS), BF16),
                pltpu.VMEM((4 * GROUPS, HEAD_DIM, COLS), BF16),
                pltpu.VMEM((HEAD_DIM, HEAD_DIM), F32),
                pltpu.VMEM((HEAD_DIM, HEAD_DIM), F32),
                pltpu.VMEM((ALL_KEYS, COLS), F32),
                pltpu.VMEM((ALL_KEYS, COLS), F32),
                pltpu.VMEM((8, COLS), F32),
                pltpu.VMEM((8, COLS), F32),
                pltpu.VMEM((2 * GROUPS, MSG, COLS), F32),
                pltpu.VMEM((2 * GROUPS, MSG, COLS), F32),
                pltpu.VMEM((2 * GROUPS, MSG, COLS), F32),
                pltpu.VMEM((GROUPS, MSG, COLS), F32),
                pltpu.VMEM((ROWS, 4096), BF16),
                dma, dma((3,)), dma((3,)), dma((GROUPS,)), dma((2,)), dma((2,)), dma((2, GROUPS)), dma((GROUPS,)),
                dma((2 * GROUPS,)), dma((2 * GROUPS,)), dma((GROUPS,)), dma((GROUPS,)),
            ],
            compiler_params=pltpu.CompilerParams(collective_id=0, has_side_effects=True,
                                                 vmem_limit_bytes=67043328),
        )(x_rows, k_cache, v_cache, ln_gain, w_q, w_k, w_v, w_o,
          q_gain.reshape(1, -1), k_gain.reshape(1, -1), jnp.asarray(cos), jnp.asarray(sin))
        return pl.pallas_call(
            hand_over, out_shape=tuple(jax.ShapeDtypeStruct(r.shape, r.dtype) for r in results),
            in_specs=[vmem_spec] * 3, out_specs=(vmem_spec,) * 3)(*results)

    return jax.shard_map(device_step, mesh=mesh,
                         in_specs=(row_spec, cache_spec, cache_spec, whole, whole, whole, whole, whole, whole, whole),
                         out_specs=(row_spec, cache_spec, cache_spec), check_vma=False)
```

```python
import functools

import jax
import jax.numpy as jnp
import numpy as np
from jax import lax
from jax.experimental import pallas as pl
from jax.experimental.pallas import tpu as pltpu
from jax.sharding import PartitionSpec as P

HEAD_DIM = 128
HALF = HEAD_DIM // 2
ROPE_THETA = 1.0e6
NORM_EPS = 1.0e-6
LOG2E = 1.4426950408889634
SCALE2 = HEAD_DIM ** -0.5 * LOG2E
MESH = pl.DeviceIdType.MESH
F32 = jnp.float32
BF16 = jnp.bfloat16
ROWS = 64
CP = 4
KEYS = 4096
ALL_KEYS = KEYS + ROWS
KV = 4
GROUPS = 8
COLS = 256
TILE = 256
MSG = HEAD_DIM + 8
HIDDEN = 2048
CHUNK = 512
FORWARD_AT = 4
EARLY = 8
VMEM_LIMIT = 60 * 1024 * 1024
EARLY_OUT = 6


def rope_tables(prefix_len):
    freq = (ROPE_THETA ** (-np.arange(HALF, dtype=np.float64) * (2.0 / HEAD_DIM))).astype(np.float32)
    pos = (prefix_len + np.arange(CP * ROWS)).astype(np.float32).reshape(CP, 1, ROWS)
    angles = (pos * freq[None, :, None]).astype(np.float32)
    angles = np.concatenate([angles, angles], axis=2).astype(np.float64)
    return np.cos(angles).astype(np.float32), np.sin(angles).astype(np.float32)


def kernel(x_hbm, k_hbm, v_hbm, ln_hbm, wq_hbm, wk_hbm, wv_hbm, wo_hbm, qg_hbm, kg_hbm, cos_hbm, sin_hbm,
           out_ref, knew_ref, vnew_ref,
           ln_ref, qg_ref, kg_ref, cos_ref, sin_ref, xall, hbuf, wbuf, ks, vt, qt, gq, gk, m_a, m_b,
           abuf, bbuf, rbuf, cbuf, obuf, part_out,
           x_sem, xs_sem, xr_sem, w_sem, kv_sem, tab_sem, cache_sem, wo_sem, as_sem, ar_sem, cs_sem, cr_sem):
    me = lax.axis_index("cp")
    dp = lax.axis_index("dp")
    partner = me + 1 - 2 * lax.rem(me, 2)
    cross = lax.rem(me + 2, CP)
    far = lax.rem(partner + 2, CP)

    def remote(src, dst, ssem, rsem, to):
        return pltpu.make_async_remote_copy(src_ref=src, dst_ref=dst, send_sem=ssem, recv_sem=rsem,
                                            device_id=(dp, to), device_id_type=MESH)

    x_copy = pltpu.make_async_copy(x_hbm, xall.at[0], x_sem)
    x_copy.start()
    small = [pltpu.make_async_copy(src, dst, tab_sem.at[n]) for n, (src, dst) in enumerate(
        ((ln_hbm, ln_ref), (qg_hbm, qg_ref), (kg_hbm, kg_ref), (cos_hbm, cos_ref), (sin_hbm, sin_ref)))]

    def wq_copy(g):
        return pltpu.make_async_copy(wq_hbm.at[:, pl.ds(pl.multiple_of(g * 512, 512), 512)], wbuf.at[g], w_sem.at[g])

    def wo_copy(b):
        nb = b // 2
        kh = b % 2
        return pltpu.make_async_copy(wo_hbm.at[pl.ds(kh * 2048, 2048), pl.ds(nb * 512, 512)], wbuf.at[b], wo_sem.at[b])

    x_to_cross = remote(xall.at[0], xall.at[2], xs_sem.at[1], xr_sem.at[1], cross)
    x_to_partner = remote(xall.at[0], xall.at[1], xs_sem.at[0], xr_sem.at[0], partner)
    x_forward = remote(xall.at[2], xall.at[3], xs_sem.at[2], xr_sem.at[2], partner)

    def normalise(slot):
        wide = xall[slot].astype(F32)
        mean_sq = jnp.mean(wide * wide, axis=-1, keepdims=True)
        ln_gain = ln_ref[...].astype(F32).reshape(1, HIDDEN)
        hbuf[slot * ROWS:(slot + 1) * ROWS, :] = (wide * lax.rsqrt(mean_sq + NORM_EPS) * ln_gain).astype(BF16)

    def norm_rope(raw_t, gain, cos, sin):
        z = raw_t.astype(F32)
        mean_sq = jnp.mean(z * z, axis=0, keepdims=True)
        y = z * lax.rsqrt(mean_sq + NORM_EPS) * gain
        first, second = y[:HALF], y[HALF:]
        return jnp.concatenate([first * cos - second * sin, second * cos + first * sin], axis=0).astype(BF16)

    def place(i):
        own = jnp.logical_or(i < 2, i >= GROUPS + 2)
        return jnp.where(i < 2, i, jnp.where(i < GROUPS + 2, i - 2, i - GROUPS)), own

    def project(i):
        g, own = place(i)
        ids = jnp.where(own, me, cross), jnp.where(own, partner, far)
        units = 2 * i + 1, 2 * i
        rows = pl.ds(pl.multiple_of(jnp.where(own, 0, 2 * ROWS), 2 * ROWS), 2 * ROWS)
        raw = jnp.dot(hbuf[rows, :], wbuf[g], preferred_element_type=F32).astype(BF16)
        for n in range(2):
            cos, sin = cos_ref[ids[n]], sin_ref[ids[n]]
            part = raw[n * ROWS:(n + 1) * ROWS]
            for hh in range(2):
                two = jnp.concatenate([part[:, hh * 256:hh * 256 + 128], part[:, hh * 256 + 128:hh * 256 + 256]], axis=0)
                qt[units[n], :, hh * 128:(hh + 1) * 128] = norm_rope(two.T, gq[...], cos, sin)

    def prologue(wk, wv, kst, vst, kf, vf):
        def cache_copy(src, dst, j, n):
            at = pl.ds(pl.multiple_of(j * CHUNK * KV, CHUNK * KV), CHUNK * KV)
            return pltpu.make_async_copy(src.at[at], dst.at[at], cache_sem.at[n, j])

        wk_copy = pltpu.make_async_copy(wk_hbm, wk, kv_sem.at[0])
        wv_copy = pltpu.make_async_copy(wv_hbm, wv, kv_sem.at[1])
        for j in range(EARLY):
            cache_copy(k_hbm, kst, j, 0).start()
            cache_copy(v_hbm, vst, j, 1).start()

        barrier = pltpu.get_barrier_semaphore()
        for to in (partner, cross):
            pl.semaphore_signal(barrier, inc=1, device_id=(dp, to), device_id_type=MESH)
        pl.semaphore_wait(barrier, 2)
        x_copy.wait()
        x_to_cross.start()
        x_to_partner.start()
        for c in small:
            c.start()
        for j in range(EARLY, GROUPS):
            cache_copy(k_hbm, kst, j, 0).start()
            cache_copy(v_hbm, vst, j, 1).start()
        wk_copy.start()
        wv_copy.start()
        for g in range(GROUPS):
            wq_copy(g).start()

        def relayout(j, carry):
            cache_copy(k_hbm, kst, j, 0).wait()
            cache_copy(v_hbm, vst, j, 1).wait()
            at = pl.ds(pl.multiple_of(j * CHUNK * KV, CHUNK * KV), CHUNK * KV)
            to = pl.ds(pl.multiple_of(j * CHUNK, CHUNK), CHUNK)
            kf[...] = kst[at].astype(F32)
            vf[...] = vst[at].astype(F32)
            for h in range(KV):
                ks[h, to, :] = kf[pl.ds(h, CHUNK, stride=KV), :].astype(BF16)
                vt[h, :, to] = vf[pl.ds(h, CHUNK, stride=KV), :].astype(BF16).T
            return carry

        lax.fori_loop(0, GROUPS, relayout, 0)

        for c in small:
            c.wait()
        gq[...] = jnp.broadcast_to(qg_ref[...].astype(F32), (HEAD_DIM, HEAD_DIM)).T
        gk[...] = jnp.broadcast_to(kg_ref[...].astype(F32), (HEAD_DIM, HEAD_DIM)).T
        normalise(0)
        x_to_partner.wait_recv()
        normalise(1)

        wk_copy.wait()
        wv_copy.wait()
        k_raw = jnp.dot(hbuf[0:ROWS, :], wk[...], preferred_element_type=F32).astype(BF16)
        v_raw = jnp.dot(hbuf[0:ROWS, :], wv[...], preferred_element_type=F32).astype(BF16)
        for hh in range(2):
            two = jnp.concatenate([k_raw[:, hh * 256:hh * 256 + 128], k_raw[:, hh * 256 + 128:hh * 256 + 256]], axis=0)
            back = norm_rope(two.T, gk[...], cos_ref[me], sin_ref[me]).T
            for n in range(2):
                ks[2 * hh + n, KEYS:ALL_KEYS, :] = back[n * ROWS:(n + 1) * ROWS]
                knew_ref[:, 2 * hh + n, :] = back[n * ROWS:(n + 1) * ROWS]
        for h in range(KV):
            one = v_raw[:, h * 128:(h + 1) * 128]
            vt[h, :, KEYS:ALL_KEYS] = one.T
            vnew_ref[:, h, :] = one

    def main(s_a, s_b):
        for g in range(2):
            wq_copy(g).wait()
            project(g)

        tiles = [(t * TILE, TILE) for t in range(KEYS // TILE)] + [(KEYS, ROWS)]

        def colmax(s, n):
            return jnp.max(s.reshape(n // 8, 8, COLS), axis=0)

        class Unit:
            pass

        def begin(u, s_ref, m_ref, dest):
            z = Unit()
            z.s, z.m = s_ref, m_ref
            z.peak = m_ref[0:1]
            z.head = place(u // 2)[0] // 2
            z.acc = z.sum = None
            return z

        def begin_next(z, u, s_ref, m_ref, dest):
            z.s, z.m = s_ref, m_ref
            z.next_head = place(u // 2)[0] // 2
            z.q = qt[u]
            z.dest = dest
            z.top = None
            return z

        def weigh(z, t):
            lo, n = tiles[t]
            p = jnp.exp2(z.s[lo:lo + n, :] * SCALE2 - z.peak)
            part = jnp.sum(p.reshape(n // 8, 8, COLS), axis=0)
            z.sum = part if z.sum is None else z.sum + part
            a = jnp.dot(vt[z.head, :, lo:lo + n], p.astype(BF16), preferred_element_type=F32)
            z.acc = a if z.acc is None else z.acc + a

        def score(z, t):
            lo, n = tiles[t]
            s = jnp.dot(ks[z.next_head, lo:lo + n, :], z.q, preferred_element_type=F32)
            if t == len(tiles) - 1:
                key = me * ROWS + lax.broadcasted_iota(jnp.int32, (n, COLS), 0)
                row = z.dest * ROWS + (lax.broadcasted_iota(jnp.int32, (n, COLS), 1) & (ROWS - 1))
                s = jnp.where(key <= row, s, -jnp.inf)
            z.s[lo:lo + n, :] = s
            top = colmax(s, n)
            z.top = top if z.top is None else jnp.maximum(z.top, top)

        def end_next(z):
            z.m[0:1] = jnp.max(z.top, axis=0, keepdims=True) * SCALE2

        def finish(z, ref, slot):
            ref[slot, 0:HEAD_DIM, :] = z.acc
            ref[slot, HEAD_DIM:HEAD_DIM + 1, :] = z.peak
            ref[slot, HEAD_DIM + 1:HEAD_DIM + 2, :] = jnp.sum(z.sum, axis=0, keepdims=True)

        def dests(i):
            own = place(i)[1]
            return jnp.where(own, partner, far), jnp.where(own, me, cross)

        za, zb = Unit(), Unit()
        da, db = partner, me
        begin_next(za, 0, s_a, m_a, da)
        begin_next(zb, 1, s_b, m_b, db)
        for t in range(len(tiles)):
            score(za, t)
            score(zb, t)
        end_next(za)
        end_next(zb)

        def to_partner(i):
            return remote(abuf.at[i], rbuf.at[i], as_sem.at[i], ar_sem.at[i], partner)

        def to_cross(g):
            return remote(bbuf.at[g + 2], cbuf.at[g], cs_sem.at[g], cr_sem.at[g], cross)

        def combine_cross(g):
            n = g + 2
            to_partner(n).wait_recv()
            m1, m2 = bbuf[n, 128:129, :], rbuf[n, 128:129, :]
            m = jnp.maximum(m1, m2)
            w1, w2 = jnp.exp2(m1 - m), jnp.exp2(m2 - m)
            bbuf[n, 0:128, :] = bbuf[n, 0:128, :] * w1 + rbuf[n, 0:128, :] * w2
            total = bbuf[n, 129:130, :] * w1 + rbuf[n, 129:130, :] * w2
            bbuf[n, 128:129, :] = m
            bbuf[n, 129:130, :] = total
            to_cross(g).start()

        def attend(i, last, ahead=False, beside=None):
            a = begin(2 * i, s_a, m_a, None)
            b = begin(2 * i + 1, s_b, m_b, None)
            if not last:
                da, db = dests(i + 1)
                begin_next(a, 2 * i + 2, s_a, m_a, da)
                begin_next(b, 2 * i + 3, s_b, m_b, db)
            for t in range(len(tiles)):
                for z in (a, b):
                    weigh(z, t)
                    if not last:
                        score(z, t)
                if ahead and t == 2:
                    project(i + 2)
                if beside is not None:
                    beside(t)
            finish(a, abuf, i)
            finish(b, bbuf, i)
            if not last:
                end_next(a)
                end_next(b)
            to_partner(i).start()

        def forward(t):
            if t == FORWARD_AT:
                x_to_cross.wait_recv()
                x_forward.start()

        def body(i, carry):
            @pl.when(jnp.logical_and(i >= 4, i < GROUPS + 4))
            def _():
                combine_cross(i - 4)

            @pl.when(jnp.logical_or(i == 2, i == 3))
            def _():
                wo_copy(i - 2).start()

            @pl.when(i >= GROUPS + 1)
            def _():
                wo_copy(i - GROUPS + 1).start()

            @pl.when(jnp.logical_and(i >= 2, i < GROUPS))
            def _():
                wq_copy(i).wait()

            attend(i, False, True)
            return carry

        attend(0, False, beside=forward)
        normalise(2)
        x_forward.wait_recv()
        normalise(3)
        project(2)
        lax.fori_loop(1, 2 * GROUPS - 2, body, 0)
        wo_copy(GROUPS - 1).start()
        attend(2 * GROUPS - 2, False)

        def slot_of(g):
            return g if g < 2 else GROUPS + g

        def arrive(g):
            to_partner(slot_of(g)).wait_recv()
            to_cross(g).wait_recv()

        def finish_group(g):
            parts = ((bbuf, slot_of(g)), (rbuf, slot_of(g)), (cbuf, g))
            peaks = [ref[n, 128:129, :] for ref, n in parts]
            m = jnp.maximum(jnp.maximum(peaks[0], peaks[1]), peaks[2])
            ws = [jnp.exp2(p - m) for p in peaks]
            total = sum(ref[n, 129:130, :] * w for (ref, n), w in zip(parts, ws))
            inv = 1.0 / total
            o = sum(ref[n, 0:128, :] * (w * inv) for (ref, n), w in zip(parts, ws)).astype(BF16)
            for hh in range(2):
                rows = o[:, hh * 128:(hh + 1) * 128].T
                for n in range(2):
                    col = (4 * g + 2 * hh + n) * HEAD_DIM
                    obuf[:, col:col + HEAD_DIM] = rows[n * ROWS:(n + 1) * ROWS]

        split = EARLY_OUT * 512

        def project_early(nb):
            cols = slice(nb * 512, (nb + 1) * 512)
            acc = jnp.dot(obuf[:, 0:2048], wbuf[2 * nb], preferred_element_type=F32)
            acc = acc + jnp.dot(obuf[:, 2048:split], wbuf[2 * nb + 1, 0:split - 2048], preferred_element_type=F32)
            part_out[:, cols] = acc

        def beside(t):
            if t < EARLY_OUT:
                finish_group(t)
            elif t in (7, 9, 11, 13):
                project_early((t - 7) // 2)

        for g in range(EARLY_OUT):
            arrive(g)
        for b in range(GROUPS):
            wo_copy(b).wait()
        attend(2 * GROUPS - 1, True, beside=beside)
        for g in range(EARLY_OUT, GROUPS):
            arrive(g)
        for g in range(EARLY_OUT, GROUPS):
            finish_group(g)
        for nb in range(4):
            cols = slice(nb * 512, (nb + 1) * 512)
            acc = jnp.dot(obuf[:, split:4096], wbuf[2 * nb + 1, split - 2048:2048], preferred_element_type=F32)
            out_ref[:, cols] = (xall[0, :, cols].astype(F32) + (part_out[:, cols] + acc)).astype(BF16)

        x_to_partner.wait_send()
        x_to_cross.wait_send()
        x_forward.wait_send()

        def drain(i, carry):
            to_partner(i).wait_send()
            return carry

        lax.fori_loop(0, 2 * GROUPS, drain, 0)

        def drain_cross(g, carry):
            to_cross(g).wait_send()
            return carry

        lax.fori_loop(0, GROUPS, drain_cross, 0)

    pl.run_scoped(
        prologue,
        pltpu.VMEM((HIDDEN, 512), BF16),
        pltpu.VMEM((HIDDEN, 512), BF16),
        pltpu.VMEM((KEYS * KV, HEAD_DIM), BF16),
        pltpu.VMEM((KEYS * KV, HEAD_DIM), BF16),
        pltpu.VMEM((CHUNK * KV, HEAD_DIM), F32),
        pltpu.VMEM((CHUNK * KV, HEAD_DIM), F32),
    )
    pl.run_scoped(main, pltpu.VMEM((ALL_KEYS, COLS), F32), pltpu.VMEM((ALL_KEYS, COLS), F32))

def hand_over(*refs):
    for src, dst in zip(refs[:3], refs[3:]):
        dst[...] = src[...]


def solution(mesh):
    row_spec = P(('dp', 'cp'), None)
    cache_spec = P(('dp', 'cp'), None, None)
    whole = P()
    any_spec = pl.BlockSpec(memory_space=pl.ANY)
    vmem_spec = pl.BlockSpec(memory_space=pltpu.VMEM)

    def device_step(x_rows, k_cache, v_cache, ln_gain, w_q, w_k, w_v, w_o, q_gain, k_gain):
        cos, sin = rope_tables(k_cache.shape[0] * CP)
        dma = pltpu.SemaphoreType.DMA
        results = pl.pallas_call(
            kernel,
            out_shape=(jax.ShapeDtypeStruct((ROWS, HIDDEN), BF16),
                       jax.ShapeDtypeStruct((ROWS, KV, HEAD_DIM), BF16),
                       jax.ShapeDtypeStruct((ROWS, KV, HEAD_DIM), BF16)),
            in_specs=[any_spec] * 12,
            out_specs=(vmem_spec, vmem_spec, vmem_spec),
            scratch_shapes=[
                pltpu.VMEM((HIDDEN,), BF16),
                pltpu.VMEM((1, HEAD_DIM), BF16),
                pltpu.VMEM((1, HEAD_DIM), BF16),
                pltpu.VMEM((CP, HALF, 128), F32),
                pltpu.VMEM((CP, HALF, 128), F32),
                pltpu.VMEM((4, ROWS, HIDDEN), BF16),
                pltpu.VMEM((4 * ROWS, HIDDEN), BF16),
                pltpu.VMEM((GROUPS, 2048, 512), BF16),
                pltpu.VMEM((KV, ALL_KEYS, HEAD_DIM), BF16),
                pltpu.VMEM((KV, HEAD_DIM, ALL_KEYS), BF16),
                pltpu.VMEM((4 * GROUPS, HEAD_DIM, COLS), BF16),
                pltpu.VMEM((HEAD_DIM, HEAD_DIM), F32),
                pltpu.VMEM((HEAD_DIM, HEAD_DIM), F32),
                pltpu.VMEM((8, COLS), F32),
                pltpu.VMEM((8, COLS), F32),
                pltpu.VMEM((2 * GROUPS, MSG, COLS), F32),
                pltpu.VMEM((2 * GROUPS, MSG, COLS), F32),
                pltpu.VMEM((2 * GROUPS, MSG, COLS), F32),
                pltpu.VMEM((GROUPS, MSG, COLS), F32),
                pltpu.VMEM((ROWS, 4096), BF16),
                pltpu.VMEM((ROWS, HIDDEN), F32),
                dma, dma((3,)), dma((3,)), dma((GROUPS,)), dma((2,)), dma((5,)), dma((2, GROUPS)), dma((GROUPS,)),
                dma((2 * GROUPS,)), dma((2 * GROUPS,)), dma((GROUPS,)), dma((GROUPS,)),
            ],
            compiler_params=pltpu.CompilerParams(collective_id=0, has_side_effects=True,
                                                 vmem_limit_bytes=VMEM_LIMIT),
        )(x_rows, k_cache.reshape(-1, HEAD_DIM), v_cache.reshape(-1, HEAD_DIM), ln_gain, w_q, w_k, w_v, w_o,
          q_gain.reshape(1, -1), k_gain.reshape(1, -1), jnp.asarray(cos), jnp.asarray(sin))
        return pl.pallas_call(
            hand_over, out_shape=tuple(jax.ShapeDtypeStruct(r.shape, r.dtype) for r in results),
            in_specs=[vmem_spec] * 3, out_specs=(vmem_spec,) * 3)(*results)

    return jax.shard_map(device_step, mesh=mesh,
                         in_specs=(row_spec, cache_spec, cache_spec, whole, whole, whole, whole, whole, whole, whole),
                         out_specs=(row_spec, cache_spec, cache_spec), check_vma=False)
```

```python
import functools

import jax
import jax.numpy as jnp
import numpy as np
from jax import lax
from jax.experimental import pallas as pl
from jax.experimental.pallas import tpu as pltpu
from jax.sharding import PartitionSpec as P

HEAD_DIM = 128
HALF = HEAD_DIM // 2
ROPE_THETA = 1.0e6
NORM_EPS = 1.0e-6
LOG2E = 1.4426950408889634
SCALE2 = HEAD_DIM ** -0.5 * LOG2E
MESH = pl.DeviceIdType.MESH
F32 = jnp.float32
BF16 = jnp.bfloat16
ROWS = 64
CP = 4
KEYS = 4096
ALL_KEYS = KEYS + ROWS
KV = 4
GROUPS = 8
COLS = 256
TILE = 256
MSG = HEAD_DIM + 8
HIDDEN = 2048
CHUNK = 512
FORWARD_AT = 2
EARLY = 8
VMEM_LIMIT = 60 * 1024 * 1024
SHARED = 6
EARLY_OUT = 6


def rope_tables(prefix_len):
    freq = (ROPE_THETA ** (-np.arange(HALF, dtype=np.float64) * (2.0 / HEAD_DIM))).astype(np.float32)
    pos = (prefix_len + np.arange(CP * ROWS)).astype(np.float32).reshape(CP, 1, ROWS)
    angles = (pos * freq[None, :, None]).astype(np.float32)
    angles = np.concatenate([angles, angles], axis=2).astype(np.float64)
    return np.cos(angles).astype(np.float32), np.sin(angles).astype(np.float32)


def kernel(x_hbm, k_hbm, v_hbm, ln_hbm, wq_hbm, wk_hbm, wv_hbm, wo_hbm, qg_hbm, kg_hbm, cos_hbm, sin_hbm,
           out_ref, knew_ref, vnew_ref,
           ln_ref, qg_ref, kg_ref, cos_ref, sin_ref, xall, hbuf, wbuf, ks, vt, qt, gq, gk, m_a, m_b,
           abuf, bbuf, rbuf, cbuf, obuf, part_out,
           x_sem, xs_sem, xr_sem, w_sem, kv_sem, tab_sem, cache_sem, wo_sem, as_sem, ar_sem, cs_sem, cr_sem, qs_sem, qr_sem):
    me = lax.axis_index("cp")
    dp = lax.axis_index("dp")
    core = lax.rem(me, 2)
    partner = me + 1 - 2 * core
    cross = lax.rem(me + 2, CP)
    far = lax.rem(partner + 2, CP)

    def remote(src, dst, ssem, rsem, to):
        return pltpu.make_async_remote_copy(src_ref=src, dst_ref=dst, send_sem=ssem, recv_sem=rsem,
                                            device_id=(dp, to), device_id_type=MESH)

    x_copy = pltpu.make_async_copy(x_hbm, xall.at[0], x_sem)
    x_copy.start()
    small = [pltpu.make_async_copy(src, dst, tab_sem.at[n]) for n, (src, dst) in enumerate(
        ((ln_hbm, ln_ref), (qg_hbm, qg_ref), (kg_hbm, kg_ref), (cos_hbm, cos_ref), (sin_hbm, sin_ref)))]

    def wq_copy(g):
        return pltpu.make_async_copy(wq_hbm.at[:, pl.ds(pl.multiple_of(g * 512, 512), 512)], wbuf.at[g], w_sem.at[g])

    def wo_copy(b):
        nb = b // 2
        kh = b % 2
        return pltpu.make_async_copy(wo_hbm.at[pl.ds(kh * 2048, 2048), pl.ds(nb * 512, 512)], wbuf.at[b], wo_sem.at[b])

    x_to_cross = remote(xall.at[0], xall.at[2], xs_sem.at[1], xr_sem.at[1], cross)
    x_to_partner = remote(xall.at[0], xall.at[1], xs_sem.at[0], xr_sem.at[0], partner)
    x_forward = remote(xall.at[2], xall.at[3], xs_sem.at[2], xr_sem.at[2], partner)

    def normalise(slot):
        wide = xall[slot].astype(F32)
        mean_sq = jnp.mean(wide * wide, axis=-1, keepdims=True)
        ln_gain = ln_ref[...].astype(F32).reshape(1, HIDDEN)
        hbuf[slot * ROWS:(slot + 1) * ROWS, :] = (wide * lax.rsqrt(mean_sq + NORM_EPS) * ln_gain).astype(BF16)

    def norm_rope(raw_t, gain, cos, sin):
        z = raw_t.astype(F32)
        mean_sq = jnp.mean(z * z, axis=0, keepdims=True)
        y = z * lax.rsqrt(mean_sq + NORM_EPS) * gain
        first, second = y[:HALF], y[HALF:]
        return jnp.concatenate([first * cos - second * sin, second * cos + first * sin], axis=0).astype(BF16)

    def place(i):
        own = jnp.logical_or(i < 2, i >= GROUPS + 2)
        return jnp.where(i < 2, i, jnp.where(i < GROUPS + 2, i - 2, i - GROUPS)), own

    def project(i):
        g, own = place(i)
        ids = jnp.where(own, me, cross), jnp.where(own, partner, far)
        units = 2 * i + 1, 2 * i
        rows = pl.ds(pl.multiple_of(jnp.where(own, 0, 2 * ROWS), 2 * ROWS), 2 * ROWS)
        raw = jnp.dot(hbuf[rows, :], wbuf[g], preferred_element_type=F32).astype(BF16)
        for n in range(2):
            cos, sin = cos_ref[ids[n]], sin_ref[ids[n]]
            part = raw[n * ROWS:(n + 1) * ROWS]
            for hh in range(2):
                two = jnp.concatenate([part[:, hh * 256:hh * 256 + 128], part[:, hh * 256 + 128:hh * 256 + 256]], axis=0)
                qt[units[n], :, hh * 128:(hh + 1) * 128] = norm_rope(two.T, gq[...], cos, sin)

    def prologue(wk, wv, kst, vst, kf, vf):
        def cache_copy(src, dst, j, n):
            at = pl.ds(pl.multiple_of(j * CHUNK * KV, CHUNK * KV), CHUNK * KV)
            return pltpu.make_async_copy(src.at[at], dst.at[at], cache_sem.at[n, j])

        wk_copy = pltpu.make_async_copy(wk_hbm, wk, kv_sem.at[0])
        wv_copy = pltpu.make_async_copy(wv_hbm, wv, kv_sem.at[1])
        for j in range(EARLY):
            cache_copy(k_hbm, kst, j, 0).start()
            cache_copy(v_hbm, vst, j, 1).start()

        barrier = pltpu.get_barrier_semaphore()
        for to in (partner, cross):
            pl.semaphore_signal(barrier, inc=1, device_id=(dp, to), device_id_type=MESH)
        pl.semaphore_wait(barrier, 2)
        x_copy.wait()
        x_to_cross.start()
        x_to_partner.start()
        for c in small:
            c.start()
        for j in range(EARLY, GROUPS):
            cache_copy(k_hbm, kst, j, 0).start()
            cache_copy(v_hbm, vst, j, 1).start()
        wk_copy.start()
        wv_copy.start()
        for g in range(2):
            wq_copy(g).start()
        for m in range(1, 4):
            wq_copy(2 * m + core).start()
        for m in range(1, 4):
            wo_copy(2 * m + 1 - core).start()

        def relayout(j, carry):
            cache_copy(k_hbm, kst, j, 0).wait()
            cache_copy(v_hbm, vst, j, 1).wait()
            at = pl.ds(pl.multiple_of(j * CHUNK * KV, CHUNK * KV), CHUNK * KV)
            to = pl.ds(pl.multiple_of(j * CHUNK, CHUNK), CHUNK)
            kf[...] = kst[at].astype(F32)
            vf[...] = vst[at].astype(F32)
            for h in range(KV):
                ks[h, to, :] = kf[pl.ds(h, CHUNK, stride=KV), :].astype(BF16)
                vt[h, :, to] = vf[pl.ds(h, CHUNK, stride=KV), :].astype(BF16).T
            return carry

        lax.fori_loop(0, GROUPS, relayout, 0)

        for c in small:
            c.wait()
        gq[...] = jnp.broadcast_to(qg_ref[...].astype(F32), (HEAD_DIM, HEAD_DIM)).T
        gk[...] = jnp.broadcast_to(kg_ref[...].astype(F32), (HEAD_DIM, HEAD_DIM)).T
        normalise(0)
        x_to_partner.wait_recv()
        normalise(1)

        wk_copy.wait()
        wv_copy.wait()
        k_raw = jnp.dot(hbuf[0:ROWS, :], wk[...], preferred_element_type=F32).astype(BF16)
        v_raw = jnp.dot(hbuf[0:ROWS, :], wv[...], preferred_element_type=F32).astype(BF16)
        for hh in range(2):
            two = jnp.concatenate([k_raw[:, hh * 256:hh * 256 + 128], k_raw[:, hh * 256 + 128:hh * 256 + 256]], axis=0)
            back = norm_rope(two.T, gk[...], cos_ref[me], sin_ref[me]).T
            for n in range(2):
                ks[2 * hh + n, KEYS:ALL_KEYS, :] = back[n * ROWS:(n + 1) * ROWS]
                knew_ref[:, 2 * hh + n, :] = back[n * ROWS:(n + 1) * ROWS]
        for h in range(KV):
            one = v_raw[:, h * 128:(h + 1) * 128]
            vt[h, :, KEYS:ALL_KEYS] = one.T
            vnew_ref[:, h, :] = one

    def main(s_a, s_b):
        for g in range(2):
            wq_copy(g).wait()
            project(g)

        tiles = [(t * TILE, TILE) for t in range(KEYS // TILE)] + [(KEYS, ROWS)]

        def colmax(s, n):
            return jnp.max(s.reshape(n // 8, 8, COLS), axis=0)

        class Unit:
            pass

        def begin(u, s_ref, m_ref, dest):
            z = Unit()
            z.s, z.m = s_ref, m_ref
            z.peak = m_ref[0:1]
            z.head = place(u // 2)[0] // 2
            z.acc = z.sum = None
            return z

        def begin_next(z, u, s_ref, m_ref, dest):
            z.s, z.m = s_ref, m_ref
            z.next_head = place(u // 2)[0] // 2
            z.q = qt[u]
            z.dest = dest
            z.top = None
            return z

        def weigh(z, t):
            lo, n = tiles[t]
            p = jnp.exp2(z.s[lo:lo + n, :] * SCALE2 - z.peak)
            part = jnp.sum(p.reshape(n // 8, 8, COLS), axis=0)
            z.sum = part if z.sum is None else z.sum + part
            a = jnp.dot(vt[z.head, :, lo:lo + n], p.astype(BF16), preferred_element_type=F32)
            z.acc = a if z.acc is None else z.acc + a

        def score(z, t):
            lo, n = tiles[t]
            s = jnp.dot(ks[z.next_head, lo:lo + n, :], z.q, preferred_element_type=F32)
            if t == len(tiles) - 1:
                key = me * ROWS + lax.broadcasted_iota(jnp.int32, (n, COLS), 0)
                row = z.dest * ROWS + (lax.broadcasted_iota(jnp.int32, (n, COLS), 1) & (ROWS - 1))
                s = jnp.where(key <= row, s, -jnp.inf)
            z.s[lo:lo + n, :] = s
            top = colmax(s, n)
            z.top = top if z.top is None else jnp.maximum(z.top, top)

        def end_next(z):
            z.m[0:1] = jnp.max(z.top, axis=0, keepdims=True) * SCALE2

        def finish(z, ref, slot):
            ref[slot, 0:HEAD_DIM, :] = z.acc
            ref[slot, HEAD_DIM:HEAD_DIM + 1, :] = z.peak
            ref[slot, HEAD_DIM + 1:HEAD_DIM + 2, :] = jnp.sum(z.sum, axis=0, keepdims=True)

        def dests(i):
            own = place(i)[1]
            return jnp.where(own, partner, far), jnp.where(own, me, cross)

        za, zb = Unit(), Unit()
        da, db = partner, me
        begin_next(za, 0, s_a, m_a, da)
        begin_next(zb, 1, s_b, m_b, db)
        for t in range(len(tiles)):
            score(za, t)
            score(zb, t)
        end_next(za)
        end_next(zb)

        def to_partner(i):
            return remote(abuf.at[i], rbuf.at[i], as_sem.at[i], ar_sem.at[i], partner)

        def to_cross(g):
            return remote(bbuf.at[g + 2], cbuf.at[g], cs_sem.at[g], cr_sem.at[g], cross)

        def combine_cross(g):
            n = g + 2
            to_partner(n).wait_recv()
            m1, m2 = bbuf[n, 128:129, :], rbuf[n, 128:129, :]
            m = jnp.maximum(m1, m2)
            w1, w2 = jnp.exp2(m1 - m), jnp.exp2(m2 - m)
            bbuf[n, 0:128, :] = bbuf[n, 0:128, :] * w1 + rbuf[n, 0:128, :] * w2
            total = bbuf[n, 129:130, :] * w1 + rbuf[n, 129:130, :] * w2
            bbuf[n, 128:129, :] = m
            bbuf[n, 129:130, :] = total
            to_cross(g).start()

        def shared_place(m, c):
            return 4 + 2 * m + c

        def share(m, c):
            p = shared_place(m, c)
            return [remote(qt.at[2 * p + n], qt.at[2 * p + 1 - n], qs_sem.at[m, n], qr_sem.at[m, n], partner)
                    for n in range(2)]

        def attend(i, last, ahead=(), beside=None):
            a = begin(2 * i, s_a, m_a, None)
            b = begin(2 * i + 1, s_b, m_b, None)
            if not last:
                da, db = dests(i + 1)
                begin_next(a, 2 * i + 2, s_a, m_a, da)
                begin_next(b, 2 * i + 3, s_b, m_b, db)
            for t in range(len(tiles)):
                for z in (a, b):
                    weigh(z, t)
                    if not last:
                        score(z, t)
                for n, p in enumerate(ahead):
                    if t == 2 + 5 * n:
                        project(p)
                if beside is not None:
                    beside(t)
            finish(a, abuf, i)
            finish(b, bbuf, i)
            if not last:
                end_next(a)
                end_next(b)
            to_partner(i).start()

        def forward(t):
            if t == FORWARD_AT:
                x_to_cross.wait_recv()
                x_forward.start()

        def before(i):
            @pl.when(jnp.logical_and(i >= 4, i < GROUPS + 4))
            def _():
                combine_cross(i - 4)

        def body(n, carry):
            i = 2 + 2 * n
            before(i)

            @pl.when(n == 0)
            def _():
                wo_copy(0).start()
                wo_copy(1).start()

            attend(i, False)
            before(i + 1)
            for c in share(n, 1 - core):
                c.wait_recv()

            @pl.when(n < 2)
            def _():
                wq_copy(2 * (n + 2) + core).wait()

            attend(i + 1, False, ahead=(shared_place(n + 1, core),))
            for c in share(n + 1, core):
                c.start()

            @pl.when(n >= 2)
            def _():
                wo_copy(2 * (n - 1) + core).start()

            return carry

        def late_body(i, carry):
            before(i)

            @pl.when(i == 2 * GROUPS - 3)
            def _():
                for c in share(SHARED - 1, 1 - core):
                    c.wait_recv()

            attend(i, False)
            return carry

        attend(0, False, beside=forward)
        normalise(2)
        x_forward.wait_recv()
        normalise(3)
        project(2)
        wq_copy(2 + core).wait()
        attend(1, False, ahead=(3, shared_place(0, core)))
        for c in share(0, core):
            c.start()
        lax.fori_loop(0, 5, body, 0)
        lax.fori_loop(12, 15, late_body, 0)

        def slot_of(g):
            return g if g < 2 else GROUPS + g

        def arrive(g):
            to_partner(slot_of(g)).wait_recv()
            to_cross(g).wait_recv()

        def finish_group(g):
            parts = ((bbuf, slot_of(g)), (rbuf, slot_of(g)), (cbuf, g))
            peaks = [ref[n, 128:129, :] for ref, n in parts]
            m = jnp.maximum(jnp.maximum(peaks[0], peaks[1]), peaks[2])
            ws = [jnp.exp2(p - m) for p in peaks]
            total = sum(ref[n, 129:130, :] * w for (ref, n), w in zip(parts, ws))
            inv = 1.0 / total
            o = sum(ref[n, 0:128, :] * (w * inv) for (ref, n), w in zip(parts, ws)).astype(BF16)
            for hh in range(2):
                rows = o[:, hh * 128:(hh + 1) * 128].T
                for n in range(2):
                    col = (4 * g + 2 * hh + n) * HEAD_DIM
                    obuf[:, col:col + HEAD_DIM] = rows[n * ROWS:(n + 1) * ROWS]

        split = EARLY_OUT * 512

        def project_early(nb):
            cols = slice(nb * 512, (nb + 1) * 512)
            acc = jnp.dot(obuf[:, 0:2048], wbuf[2 * nb], preferred_element_type=F32)
            acc = acc + jnp.dot(obuf[:, 2048:split], wbuf[2 * nb + 1, 0:split - 2048], preferred_element_type=F32)
            part_out[:, cols] = acc

        def beside(t):
            if t < EARLY_OUT:
                finish_group(t)
            elif t in (7, 9, 11, 13):
                project_early((t - 7) // 2)

        for g in range(EARLY_OUT):
            arrive(g)
        for b in range(GROUPS):
            wo_copy(b).wait()
        attend(2 * GROUPS - 1, True, beside=beside)
        for g in range(EARLY_OUT, GROUPS):
            arrive(g)
        for g in range(EARLY_OUT, GROUPS):
            finish_group(g)
        for nb in range(4):
            cols = slice(nb * 512, (nb + 1) * 512)
            acc = jnp.dot(obuf[:, split:4096], wbuf[2 * nb + 1, split - 2048:2048], preferred_element_type=F32)
            out_ref[:, cols] = (xall[0, :, cols].astype(F32) + (part_out[:, cols] + acc)).astype(BF16)

        x_to_partner.wait_send()
        x_to_cross.wait_send()
        x_forward.wait_send()
        for m in range(SHARED):
            for c in share(m, core):
                c.wait_send()

        def drain(i, carry):
            to_partner(i).wait_send()
            return carry

        lax.fori_loop(0, 2 * GROUPS, drain, 0)

        def drain_cross(g, carry):
            to_cross(g).wait_send()
            return carry

        lax.fori_loop(0, GROUPS, drain_cross, 0)

    pl.run_scoped(
        prologue,
        pltpu.VMEM((HIDDEN, 512), BF16),
        pltpu.VMEM((HIDDEN, 512), BF16),
        pltpu.VMEM((KEYS * KV, HEAD_DIM), BF16),
        pltpu.VMEM((KEYS * KV, HEAD_DIM), BF16),
        pltpu.VMEM((CHUNK * KV, HEAD_DIM), F32),
        pltpu.VMEM((CHUNK * KV, HEAD_DIM), F32),
    )
    pl.run_scoped(main, pltpu.VMEM((ALL_KEYS, COLS), F32), pltpu.VMEM((ALL_KEYS, COLS), F32))

def hand_over(*refs):
    for src, dst in zip(refs[:3], refs[3:]):
        dst[...] = src[...]


def solution(mesh):
    row_spec = P(('dp', 'cp'), None)
    cache_spec = P(('dp', 'cp'), None, None)
    whole = P()
    any_spec = pl.BlockSpec(memory_space=pl.ANY)
    vmem_spec = pl.BlockSpec(memory_space=pltpu.VMEM)

    def device_step(x_rows, k_cache, v_cache, ln_gain, w_q, w_k, w_v, w_o, q_gain, k_gain):
        cos, sin = rope_tables(k_cache.shape[0] * CP)
        dma = pltpu.SemaphoreType.DMA
        results = pl.pallas_call(
            kernel,
            out_shape=(jax.ShapeDtypeStruct((ROWS, HIDDEN), BF16),
                       jax.ShapeDtypeStruct((ROWS, KV, HEAD_DIM), BF16),
                       jax.ShapeDtypeStruct((ROWS, KV, HEAD_DIM), BF16)),
            in_specs=[any_spec] * 12,
            out_specs=(vmem_spec, vmem_spec, vmem_spec),
            scratch_shapes=[
                pltpu.VMEM((HIDDEN,), BF16),
                pltpu.VMEM((1, HEAD_DIM), BF16),
                pltpu.VMEM((1, HEAD_DIM), BF16),
                pltpu.VMEM((CP, HALF, 128), F32),
                pltpu.VMEM((CP, HALF, 128), F32),
                pltpu.VMEM((4, ROWS, HIDDEN), BF16),
                pltpu.VMEM((4 * ROWS, HIDDEN), BF16),
                pltpu.VMEM((GROUPS, 2048, 512), BF16),
                pltpu.VMEM((KV, ALL_KEYS, HEAD_DIM), BF16),
                pltpu.VMEM((KV, HEAD_DIM, ALL_KEYS), BF16),
                pltpu.VMEM((4 * GROUPS, HEAD_DIM, COLS), BF16),
                pltpu.VMEM((HEAD_DIM, HEAD_DIM), F32),
                pltpu.VMEM((HEAD_DIM, HEAD_DIM), F32),
                pltpu.VMEM((8, COLS), F32),
                pltpu.VMEM((8, COLS), F32),
                pltpu.VMEM((2 * GROUPS, MSG, COLS), F32),
                pltpu.VMEM((2 * GROUPS, MSG, COLS), F32),
                pltpu.VMEM((2 * GROUPS, MSG, COLS), F32),
                pltpu.VMEM((GROUPS, MSG, COLS), F32),
                pltpu.VMEM((ROWS, 4096), BF16),
                pltpu.VMEM((ROWS, HIDDEN), F32),
                dma, dma((3,)), dma((3,)), dma((GROUPS,)), dma((2,)), dma((5,)), dma((2, GROUPS)), dma((GROUPS,)),
                dma((2 * GROUPS,)), dma((2 * GROUPS,)), dma((GROUPS,)), dma((GROUPS,)),
                dma((SHARED, 2)), dma((SHARED, 2)),
            ],
            compiler_params=pltpu.CompilerParams(collective_id=0, has_side_effects=True,
                                                 vmem_limit_bytes=VMEM_LIMIT),
        )(x_rows, k_cache.reshape(-1, HEAD_DIM), v_cache.reshape(-1, HEAD_DIM), ln_gain, w_q, w_k, w_v, w_o,
          q_gain.reshape(1, -1), k_gain.reshape(1, -1), jnp.asarray(cos), jnp.asarray(sin))
        return pl.pallas_call(
            hand_over, out_shape=tuple(jax.ShapeDtypeStruct(r.shape, r.dtype) for r in results),
            in_specs=[vmem_spec] * 3, out_specs=(vmem_spec,) * 3)(*results)

    return jax.shard_map(device_step, mesh=mesh,
                         in_specs=(row_spec, cache_spec, cache_spec, whole, whole, whole, whole, whole, whole, whole),
                         out_specs=(row_spec, cache_spec, cache_spec), check_vma=False)
```

```python
import functools

import jax
import jax.numpy as jnp
import numpy as np
from jax import lax
from jax.experimental import pallas as pl
from jax.experimental.pallas import tpu as pltpu
from jax.sharding import PartitionSpec as P

HEAD_DIM = 128
HALF = HEAD_DIM // 2
ROPE_THETA = 1.0e6
NORM_EPS = 1.0e-6
LOG2E = 1.4426950408889634
SCALE2 = HEAD_DIM ** -0.5 * LOG2E
MESH = pl.DeviceIdType.MESH
F32 = jnp.float32
BF16 = jnp.bfloat16
ROWS = 64
CP = 4
KEYS = 4096
ALL_KEYS = KEYS + ROWS
KV = 4
GROUPS = 8
COLS = 256
TILE = 256
MSG = HEAD_DIM + 8
HIDDEN = 2048
CHUNK = 512
FORWARD_AT = 2
EARLY = 8
VMEM_LIMIT = 60 * 1024 * 1024
SHARED = 6
EARLY_OUT = 6


def rope_tables(prefix_len):
    freq = (ROPE_THETA ** (-np.arange(HALF, dtype=np.float64) * (2.0 / HEAD_DIM))).astype(np.float32)
    pos = (prefix_len + np.arange(CP * ROWS)).astype(np.float32).reshape(CP, 1, ROWS)
    angles = (pos * freq[None, :, None]).astype(np.float32)
    angles = np.concatenate([angles, angles], axis=2).astype(np.float64)
    return np.cos(angles).astype(np.float32), np.sin(angles).astype(np.float32)


def kernel(x_hbm, k_hbm, v_hbm, ln_hbm, wq_hbm, wk_hbm, wv_hbm, wo_hbm, qg_hbm, kg_hbm, cos_hbm, sin_hbm,
           out_ref, knew_ref, vnew_ref,
           ln_ref, qg_ref, kg_ref, cos_ref, sin_ref, xall, hbuf, wbuf, ks, vt, qt, gq, gk, m_a, m_b,
           abuf, bbuf, rbuf, cbuf, obuf, part_out,
           x_sem, xs_sem, xr_sem, w_sem, kv_sem, tab_sem, cache_sem, wo_sem, as_sem, ar_sem, cs_sem, cr_sem, qs_sem, qr_sem):
    me = lax.axis_index("cp")
    dp = lax.axis_index("dp")
    core = lax.rem(me, 2)
    partner = me + 1 - 2 * core
    cross = lax.rem(me + 2, CP)
    far = lax.rem(partner + 2, CP)

    def remote(src, dst, ssem, rsem, to):
        return pltpu.make_async_remote_copy(src_ref=src, dst_ref=dst, send_sem=ssem, recv_sem=rsem,
                                            device_id=(dp, to), device_id_type=MESH)

    x_copy = pltpu.make_async_copy(x_hbm, xall.at[0], x_sem)
    x_copy.start()
    small = [pltpu.make_async_copy(src, dst, tab_sem.at[n]) for n, (src, dst) in enumerate(
        ((ln_hbm, ln_ref), (qg_hbm, qg_ref), (kg_hbm, kg_ref), (cos_hbm, cos_ref), (sin_hbm, sin_ref)))]

    def wq_copy(g):
        return pltpu.make_async_copy(wq_hbm.at[:, pl.ds(pl.multiple_of(g * 512, 512), 512)], wbuf.at[g], w_sem.at[g])

    def wo_copy(b):
        nb = b // 2
        kh = b % 2
        return pltpu.make_async_copy(wo_hbm.at[pl.ds(kh * 2048, 2048), pl.ds(nb * 512, 512)], wbuf.at[b], wo_sem.at[b])

    x_to_cross = remote(xall.at[0], xall.at[2], xs_sem.at[1], xr_sem.at[1], cross)
    x_to_partner = remote(xall.at[0], xall.at[1], xs_sem.at[0], xr_sem.at[0], partner)
    x_forward = remote(xall.at[2], xall.at[3], xs_sem.at[2], xr_sem.at[2], partner)

    def normalise(slot):
        wide = xall[slot].astype(F32)
        mean_sq = jnp.mean(wide * wide, axis=-1, keepdims=True)
        ln_gain = ln_ref[...].astype(F32).reshape(1, HIDDEN)
        hbuf[slot * ROWS:(slot + 1) * ROWS, :] = (wide * lax.rsqrt(mean_sq + NORM_EPS) * ln_gain).astype(BF16)

    def norm_rope(raw_t, gain, cos, sin):
        z = raw_t.astype(F32)
        mean_sq = jnp.mean(z * z, axis=0, keepdims=True)
        y = z * lax.rsqrt(mean_sq + NORM_EPS) * gain
        first, second = y[:HALF], y[HALF:]
        return jnp.concatenate([first * cos - second * sin, second * cos + first * sin], axis=0).astype(BF16)

    def place(i):
        own = jnp.logical_or(i < 2, i >= GROUPS + 2)
        return jnp.where(i < 2, i, jnp.where(i < GROUPS + 2, i - 2, i - GROUPS)), own

    def project(i):
        g, own = place(i)
        ids = jnp.where(own, me, cross), jnp.where(own, partner, far)
        units = 2 * i + 1, 2 * i
        rows = pl.ds(pl.multiple_of(jnp.where(own, 0, 2 * ROWS), 2 * ROWS), 2 * ROWS)
        raw = jnp.dot(hbuf[rows, :], wbuf[g], preferred_element_type=F32).astype(BF16)
        for n in range(2):
            cos, sin = cos_ref[ids[n]], sin_ref[ids[n]]
            part = raw[n * ROWS:(n + 1) * ROWS]
            for hh in range(2):
                two = jnp.concatenate([part[:, hh * 256:hh * 256 + 128], part[:, hh * 256 + 128:hh * 256 + 256]], axis=0)
                qt[units[n], :, hh * 128:(hh + 1) * 128] = norm_rope(two.T, gq[...], cos, sin)

    def prologue(wk, wv, kst, vst, kf, vf):
        def cache_copy(src, dst, j, n):
            at = pl.ds(pl.multiple_of(j * CHUNK * KV, CHUNK * KV), CHUNK * KV)
            return pltpu.make_async_copy(src.at[at], dst.at[at], cache_sem.at[n, j])

        wk_copy = pltpu.make_async_copy(wk_hbm, wk, kv_sem.at[0])
        wv_copy = pltpu.make_async_copy(wv_hbm, wv, kv_sem.at[1])
        for j in range(EARLY):
            cache_copy(k_hbm, kst, j, 0).start()
            cache_copy(v_hbm, vst, j, 1).start()

        barrier = pltpu.get_barrier_semaphore()
        for to in (partner, cross):
            pl.semaphore_signal(barrier, inc=1, device_id=(dp, to), device_id_type=MESH)
        pl.semaphore_wait(barrier, 2)
        x_copy.wait()
        x_to_cross.start()
        x_to_partner.start()
        for c in small:
            c.start()
        for j in range(EARLY, GROUPS):
            cache_copy(k_hbm, kst, j, 0).start()
            cache_copy(v_hbm, vst, j, 1).start()
        wk_copy.start()
        wv_copy.start()
        for g in range(2):
            wq_copy(g).start()
        for m in range(1, 4):
            wq_copy(2 * m + core).start()
        for m in range(1, 4):
            wo_copy(2 * m + 1 - core).start()

        def relayout(j, carry):
            cache_copy(k_hbm, kst, j, 0).wait()
            cache_copy(v_hbm, vst, j, 1).wait()
            at = pl.ds(pl.multiple_of(j * CHUNK * KV, CHUNK * KV), CHUNK * KV)
            to = pl.ds(pl.multiple_of(j * CHUNK, CHUNK), CHUNK)
            kf[...] = kst[at].astype(F32)
            vf[...] = vst[at].astype(F32)
            for h in range(KV):
                ks[h, to, :] = kf[pl.ds(h, CHUNK, stride=KV), :].astype(BF16)
                vt[h, :, to] = vf[pl.ds(h, CHUNK, stride=KV), :].astype(BF16).T
            return carry

        lax.fori_loop(0, GROUPS, relayout, 0)

        for c in small:
            c.wait()
        gq[...] = jnp.broadcast_to(qg_ref[...].astype(F32), (HEAD_DIM, HEAD_DIM)).T
        gk[...] = jnp.broadcast_to(kg_ref[...].astype(F32), (HEAD_DIM, HEAD_DIM)).T
        normalise(0)
        x_to_partner.wait_recv()
        normalise(1)

        wk_copy.wait()
        wv_copy.wait()
        k_raw = jnp.dot(hbuf[0:ROWS, :], wk[...], preferred_element_type=F32).astype(BF16)
        v_raw = jnp.dot(hbuf[0:ROWS, :], wv[...], preferred_element_type=F32).astype(BF16)
        for hh in range(2):
            two = jnp.concatenate([k_raw[:, hh * 256:hh * 256 + 128], k_raw[:, hh * 256 + 128:hh * 256 + 256]], axis=0)
            back = norm_rope(two.T, gk[...], cos_ref[me], sin_ref[me]).T
            for n in range(2):
                ks[2 * hh + n, KEYS:ALL_KEYS, :] = back[n * ROWS:(n + 1) * ROWS]
                knew_ref[:, 2 * hh + n, :] = back[n * ROWS:(n + 1) * ROWS]
        for h in range(KV):
            one = v_raw[:, h * 128:(h + 1) * 128]
            vt[h, :, KEYS:ALL_KEYS] = one.T
            vnew_ref[:, h, :] = one

    def main(s_a, s_b):
        for g in range(2):
            wq_copy(g).wait()
            project(g)

        tiles = [(t * TILE, TILE) for t in range(KEYS // TILE)] + [(KEYS, ROWS)]

        def colmax(s, n):
            return jnp.max(s.reshape(n // 8, 8, COLS), axis=0)

        class Unit:
            pass

        def begin(u, s_ref, m_ref, dest):
            z = Unit()
            z.s, z.m = s_ref, m_ref
            z.peak = m_ref[0:1]
            z.head = place(u // 2)[0] // 2
            z.acc = z.sum = None
            return z

        def begin_next(z, u, s_ref, m_ref, dest):
            z.s, z.m = s_ref, m_ref
            z.next_head = place(u // 2)[0] // 2
            z.q = qt[u]
            z.dest = dest
            z.top = None
            return z

        def weigh(z, t):
            lo, n = tiles[t]
            p = jnp.exp2(z.s[lo:lo + n, :] * SCALE2 - z.peak)
            part = jnp.sum(p.reshape(n // 8, 8, COLS), axis=0)
            z.sum = part if z.sum is None else z.sum + part
            a = jnp.dot(vt[z.head, :, lo:lo + n], p.astype(BF16), preferred_element_type=F32)
            z.acc = a if z.acc is None else z.acc + a

        def score(z, t):
            lo, n = tiles[t]
            s = jnp.dot(ks[z.next_head, lo:lo + n, :], z.q, preferred_element_type=F32)
            if t == len(tiles) - 1:
                key = me * ROWS + lax.broadcasted_iota(jnp.int32, (n, COLS), 0)
                row = z.dest * ROWS + (lax.broadcasted_iota(jnp.int32, (n, COLS), 1) & (ROWS - 1))
                s = jnp.where(key <= row, s, -jnp.inf)
            z.s[lo:lo + n, :] = s
            top = colmax(s, n)
            z.top = top if z.top is None else jnp.maximum(z.top, top)

        def end_next(z):
            z.m[0:1] = jnp.max(z.top, axis=0, keepdims=True) * SCALE2

        def finish(z, ref, slot):
            ref[slot, 0:HEAD_DIM, :] = z.acc
            ref[slot, HEAD_DIM:HEAD_DIM + 1, :] = z.peak
            ref[slot, HEAD_DIM + 1:HEAD_DIM + 2, :] = jnp.sum(z.sum, axis=0, keepdims=True)

        def dests(i):
            own = place(i)[1]
            return jnp.where(own, partner, far), jnp.where(own, me, cross)

        za, zb = Unit(), Unit()
        da, db = partner, me
        begin_next(za, 0, s_a, m_a, da)
        begin_next(zb, 1, s_b, m_b, db)
        for t in range(len(tiles)):
            score(za, t)
            score(zb, t)
        end_next(za)
        end_next(zb)

        def to_partner(i):
            return remote(abuf.at[i], rbuf.at[i], as_sem.at[i], ar_sem.at[i], partner)

        def to_cross(g):
            return remote(bbuf.at[g + 2], cbuf.at[g], cs_sem.at[g], cr_sem.at[g], cross)

        def combine_cross(g):
            n = g + 2
            to_partner(n).wait_recv()
            m1, m2 = bbuf[n, 128:129, :], rbuf[n, 128:129, :]
            m = jnp.maximum(m1, m2)
            w1, w2 = jnp.exp2(m1 - m), jnp.exp2(m2 - m)
            bbuf[n, 0:128, :] = bbuf[n, 0:128, :] * w1 + rbuf[n, 0:128, :] * w2
            total = bbuf[n, 129:130, :] * w1 + rbuf[n, 129:130, :] * w2
            bbuf[n, 128:129, :] = m
            bbuf[n, 129:130, :] = total
            to_cross(g).start()

        def shared_place(m, c):
            return 4 + 2 * m + c

        def share(m, c):
            p = shared_place(m, c)
            return [remote(qt.at[2 * p + n], qt.at[2 * p + 1 - n], qs_sem.at[m, n], qr_sem.at[m, n], partner)
                    for n in range(2)]

        def attend(i, last, ahead=(), beside=None):
            a = begin(2 * i, s_a, m_a, None)
            b = begin(2 * i + 1, s_b, m_b, None)
            if not last:
                da, db = dests(i + 1)
                begin_next(a, 2 * i + 2, s_a, m_a, da)
                begin_next(b, 2 * i + 3, s_b, m_b, db)
            for t in range(len(tiles)):
                for z in (a, b):
                    weigh(z, t)
                    if not last:
                        score(z, t)
                for n, p in enumerate(ahead):
                    if t == 2 + 5 * n:
                        project(p)
                if beside is not None:
                    beside(t)
            finish(a, abuf, i)
            finish(b, bbuf, i)
            if not last:
                end_next(a)
                end_next(b)
            to_partner(i).start()

        def forward(t):
            if t == FORWARD_AT:
                x_to_cross.wait_recv()
                x_forward.start()

        def before(i):
            @pl.when(jnp.logical_and(i >= 4, i < GROUPS + 4))
            def _():
                combine_cross(i - 4)

        def body(n, carry):
            i = 2 + 2 * n
            before(i)

            @pl.when(n == 0)
            def _():
                wo_copy(0).start()
                wo_copy(1).start()

            attend(i, False)
            before(i + 1)
            for c in share(n, 1 - core):
                c.wait_recv()

            @pl.when(n < 2)
            def _():
                wq_copy(2 * (n + 2) + core).wait()

            attend(i + 1, False, ahead=(shared_place(n + 1, core),))
            for c in share(n + 1, core):
                c.start()

            @pl.when(n >= 2)
            def _():
                wo_copy(2 * (n - 1) + core).start()

            return carry

        def late_body(i, carry):
            before(i)

            @pl.when(i == 2 * GROUPS - 3)
            def _():
                for c in share(SHARED - 1, 1 - core):
                    c.wait_recv()

            attend(i, False)
            return carry

        attend(0, False, beside=forward)
        normalise(2)
        x_forward.wait_recv()
        normalise(3)
        project(2)
        wq_copy(2 + core).wait()
        attend(1, False, ahead=(3, shared_place(0, core)))
        for c in share(0, core):
            c.start()
        lax.fori_loop(0, 5, body, 0)
        lax.fori_loop(12, 15, late_body, 0)

        def slot_of(g):
            return g if g < 2 else GROUPS + g

        def arrive(g):
            to_partner(slot_of(g)).wait_recv()
            to_cross(g).wait_recv()

        def finish_group(g):
            parts = ((bbuf, slot_of(g)), (rbuf, slot_of(g)), (cbuf, g))
            peaks = [ref[n, 128:129, :] for ref, n in parts]
            m = jnp.maximum(jnp.maximum(peaks[0], peaks[1]), peaks[2])
            ws = [jnp.exp2(p - m) for p in peaks]
            total = sum(ref[n, 129:130, :] * w for (ref, n), w in zip(parts, ws))
            inv = 1.0 / total
            o = sum(ref[n, 0:128, :] * (w * inv) for (ref, n), w in zip(parts, ws)).astype(BF16)
            for hh in range(2):
                rows = o[:, hh * 128:(hh + 1) * 128].T
                for n in range(2):
                    col = (4 * g + 2 * hh + n) * HEAD_DIM
                    obuf[:, col:col + HEAD_DIM] = rows[n * ROWS:(n + 1) * ROWS]

        split = EARLY_OUT * 512

        def project_early(nb):
            cols = slice(nb * 512, (nb + 1) * 512)
            acc = jnp.dot(obuf[:, 0:2048], wbuf[2 * nb], preferred_element_type=F32)
            acc = acc + jnp.dot(obuf[:, 2048:split], wbuf[2 * nb + 1, 0:split - 2048], preferred_element_type=F32)
            part_out[:, cols] = acc

        def beside(t):
            if t < EARLY_OUT:
                finish_group(t)
            elif t in (7, 9, 11, 13):
                project_early((t - 7) // 2)

        for g in range(EARLY_OUT):
            arrive(g)
        for b in range(GROUPS):
            wo_copy(b).wait()
        attend(2 * GROUPS - 1, True, beside=beside)
        for g in range(EARLY_OUT, GROUPS):
            arrive(g)
        for g in range(EARLY_OUT, GROUPS):
            finish_group(g)
        for nb in range(4):
            cols = slice(nb * 512, (nb + 1) * 512)
            acc = jnp.dot(obuf[:, split:4096], wbuf[2 * nb + 1, split - 2048:2048], preferred_element_type=F32)
            out_ref[:, cols] = (xall[0, :, cols].astype(F32) + (part_out[:, cols] + acc)).astype(BF16)

        x_to_partner.wait_send()
        x_to_cross.wait_send()
        x_forward.wait_send()
        for m in range(SHARED):
            for c in share(m, core):
                c.wait_send()

        def drain(i, carry):
            to_partner(i).wait_send()
            return carry

        lax.fori_loop(0, 2 * GROUPS, drain, 0)

        def drain_cross(g, carry):
            to_cross(g).wait_send()
            return carry

        lax.fori_loop(0, GROUPS, drain_cross, 0)

    pl.run_scoped(
        prologue,
        pltpu.VMEM((HIDDEN, 512), BF16),
        pltpu.VMEM((HIDDEN, 512), BF16),
        pltpu.VMEM((KEYS * KV, HEAD_DIM), BF16),
        pltpu.VMEM((KEYS * KV, HEAD_DIM), BF16),
        pltpu.VMEM((CHUNK * KV, HEAD_DIM), F32),
        pltpu.VMEM((CHUNK * KV, HEAD_DIM), F32),
    )
    pl.run_scoped(main, pltpu.VMEM((ALL_KEYS, COLS), F32), pltpu.VMEM((ALL_KEYS, COLS), F32))

def hand_over(*refs):
    for src, dst in zip(refs[:3], refs[3:]):
        dst[...] = src[...]


def solution(mesh):
    row_spec = P(('dp', 'cp'), None)
    cache_spec = P(('dp', 'cp'), None, None)
    whole = P()
    any_spec = pl.BlockSpec(memory_space=pl.ANY)
    vmem_spec = pl.BlockSpec(memory_space=pltpu.VMEM)

    def device_step(x_rows, k_cache, v_cache, ln_gain, w_q, w_k, w_v, w_o, q_gain, k_gain):
        cos, sin = rope_tables(k_cache.shape[0] * CP)
        dma = pltpu.SemaphoreType.DMA
        results = pl.pallas_call(
            kernel,
            out_shape=(pltpu.VMEM((ROWS, HIDDEN), BF16),
                       pltpu.VMEM((ROWS, KV, HEAD_DIM), BF16),
                       pltpu.VMEM((ROWS, KV, HEAD_DIM), BF16)),
            in_specs=[any_spec] * 12,
            out_specs=(vmem_spec, vmem_spec, vmem_spec),
            scratch_shapes=[
                pltpu.VMEM((HIDDEN,), BF16),
                pltpu.VMEM((1, HEAD_DIM), BF16),
                pltpu.VMEM((1, HEAD_DIM), BF16),
                pltpu.VMEM((CP, HALF, 128), F32),
                pltpu.VMEM((CP, HALF, 128), F32),
                pltpu.VMEM((4, ROWS, HIDDEN), BF16),
                pltpu.VMEM((4 * ROWS, HIDDEN), BF16),
                pltpu.VMEM((GROUPS, 2048, 512), BF16),
                pltpu.VMEM((KV, ALL_KEYS, HEAD_DIM), BF16),
                pltpu.VMEM((KV, HEAD_DIM, ALL_KEYS), BF16),
                pltpu.VMEM((4 * GROUPS, HEAD_DIM, COLS), BF16),
                pltpu.VMEM((HEAD_DIM, HEAD_DIM), F32),
                pltpu.VMEM((HEAD_DIM, HEAD_DIM), F32),
                pltpu.VMEM((8, COLS), F32),
                pltpu.VMEM((8, COLS), F32),
                pltpu.VMEM((2 * GROUPS, MSG, COLS), F32),
                pltpu.VMEM((2 * GROUPS, MSG, COLS), F32),
                pltpu.VMEM((2 * GROUPS, MSG, COLS), F32),
                pltpu.VMEM((GROUPS, MSG, COLS), F32),
                pltpu.VMEM((ROWS, 4096), BF16),
                pltpu.VMEM((ROWS, HIDDEN), F32),
                dma, dma((3,)), dma((3,)), dma((GROUPS,)), dma((2,)), dma((5,)), dma((2, GROUPS)), dma((GROUPS,)),
                dma((2 * GROUPS,)), dma((2 * GROUPS,)), dma((GROUPS,)), dma((GROUPS,)),
                dma((SHARED, 2)), dma((SHARED, 2)),
            ],
            compiler_params=pltpu.CompilerParams(collective_id=0, has_side_effects=True,
                                                 vmem_limit_bytes=VMEM_LIMIT),
        )(x_rows, k_cache.reshape(-1, HEAD_DIM), v_cache.reshape(-1, HEAD_DIM), ln_gain, w_q, w_k, w_v, w_o,
          q_gain.reshape(1, -1), k_gain.reshape(1, -1), jnp.asarray(cos), jnp.asarray(sin))
        return pl.pallas_call(
            hand_over, out_shape=tuple(jax.ShapeDtypeStruct(r.shape, r.dtype) for r in results),
            in_specs=[vmem_spec] * 3, out_specs=(vmem_spec,) * 3,
        )(*[pltpu.with_memory_space_constraint(r, pltpu.VMEM) for r in results])

    return jax.shard_map(device_step, mesh=mesh,
                         in_specs=(row_spec, cache_spec, cache_spec, whole, whole, whole, whole, whole, whole, whole),
                         out_specs=(row_spec, cache_spec, cache_spec), check_vma=False)
```

```python
import functools

import jax
import jax.numpy as jnp
import numpy as np
from jax import lax
from jax.experimental import pallas as pl
from jax.experimental.pallas import tpu as pltpu
from jax.sharding import PartitionSpec as P

HEAD_DIM = 128
HALF = HEAD_DIM // 2
ROPE_THETA = 1.0e6
NORM_EPS = 1.0e-6
LOG2E = 1.4426950408889634
SCALE2 = HEAD_DIM ** -0.5 * LOG2E
MESH = pl.DeviceIdType.MESH
F32 = jnp.float32
BF16 = jnp.bfloat16
ROWS = 64
CP = 4
KEYS = 4096
ALL_KEYS = KEYS + ROWS
KV = 4
GROUPS = 8
COLS = 256
TILE = 256
MSG = HEAD_DIM + 8
HIDDEN = 2048
CHUNK = 512
FORWARD_AT = 2
EARLY = 8
VMEM_LIMIT = 60 * 1024 * 1024
SHARED = 6
EARLY_OUT = 6


def rope_tables(prefix_len):
    freq = (ROPE_THETA ** (-np.arange(HALF, dtype=np.float64) * (2.0 / HEAD_DIM))).astype(np.float32)
    pos = (prefix_len + np.arange(CP * ROWS)).astype(np.float32).reshape(CP, 1, ROWS)
    angles = (pos * freq[None, :, None]).astype(np.float32)
    angles = np.concatenate([angles, angles], axis=2).astype(np.float64)
    return np.cos(angles).astype(np.float32), np.sin(angles).astype(np.float32)


def kernel(x_hbm, k_hbm, v_hbm, ln_hbm, wq_hbm, wk_hbm, wv_hbm, wo_hbm, qg_hbm, kg_hbm, cos_hbm, sin_hbm,
           out_ref, knew_ref, vnew_ref,
           ln_ref, qg_ref, kg_ref, cos_ref, sin_ref, xall, hbuf, wbuf, ks, vt, qt, gq, gk, m_a, m_b,
           abuf, bbuf, rbuf, cbuf, obuf, part_out,
           x_sem, xs_sem, xr_sem, w_sem, kv_sem, tab_sem, cache_sem, wo_sem, as_sem, ar_sem, cs_sem, cr_sem, qs_sem, qr_sem):
    me = lax.axis_index("cp")
    dp = lax.axis_index("dp")
    core = lax.rem(me, 2)
    partner = me + 1 - 2 * core
    cross = lax.rem(me + 2, CP)
    far = lax.rem(partner + 2, CP)

    def remote(src, dst, ssem, rsem, to):
        return pltpu.make_async_remote_copy(src_ref=src, dst_ref=dst, send_sem=ssem, recv_sem=rsem,
                                            device_id=(dp, to), device_id_type=MESH)

    x_copy = pltpu.make_async_copy(x_hbm, xall.at[0], x_sem)
    x_copy.start()
    small = [pltpu.make_async_copy(src, dst, tab_sem.at[n]) for n, (src, dst) in enumerate(
        ((ln_hbm, ln_ref), (qg_hbm, qg_ref), (kg_hbm, kg_ref), (cos_hbm, cos_ref), (sin_hbm, sin_ref)))]

    def wq_copy(g):
        return pltpu.make_async_copy(wq_hbm.at[:, pl.ds(pl.multiple_of(g * 512, 512), 512)], wbuf.at[g], w_sem.at[g])

    def wo_copy(b):
        nb = b // 2
        kh = b % 2
        return pltpu.make_async_copy(wo_hbm.at[pl.ds(kh * 2048, 2048), pl.ds(nb * 512, 512)], wbuf.at[b], wo_sem.at[b])

    x_to_cross = remote(xall.at[0], xall.at[2], xs_sem.at[1], xr_sem.at[1], cross)
    x_to_partner = remote(xall.at[0], xall.at[1], xs_sem.at[0], xr_sem.at[0], partner)
    x_forward = remote(xall.at[2], xall.at[3], xs_sem.at[2], xr_sem.at[2], partner)

    def normalise(slot):
        wide = xall[slot].astype(F32)
        mean_sq = jnp.mean(wide * wide, axis=-1, keepdims=True)
        ln_gain = ln_ref[...].astype(F32).reshape(1, HIDDEN)
        hbuf[slot * ROWS:(slot + 1) * ROWS, :] = (wide * lax.rsqrt(mean_sq + NORM_EPS) * ln_gain).astype(BF16)

    def norm_rope(raw_t, gain, cos, sin):
        z = raw_t.astype(F32)
        mean_sq = jnp.mean(z * z, axis=0, keepdims=True)
        y = z * lax.rsqrt(mean_sq + NORM_EPS) * gain
        first, second = y[:HALF], y[HALF:]
        return jnp.concatenate([first * cos - second * sin, second * cos + first * sin], axis=0).astype(BF16)

    def place(i):
        own = jnp.logical_or(i < 2, i >= GROUPS + 2)
        return jnp.where(i < 2, i, jnp.where(i < GROUPS + 2, i - 2, i - GROUPS)), own

    def project(i):
        g, own = place(i)
        ids = jnp.where(own, me, cross), jnp.where(own, partner, far)
        units = 2 * i + 1, 2 * i
        rows = pl.ds(pl.multiple_of(jnp.where(own, 0, 2 * ROWS), 2 * ROWS), 2 * ROWS)
        raw = jnp.dot(hbuf[rows, :], wbuf[g], preferred_element_type=F32).astype(BF16)
        for n in range(2):
            cos, sin = cos_ref[ids[n]], sin_ref[ids[n]]
            part = raw[n * ROWS:(n + 1) * ROWS]
            for hh in range(2):
                two = jnp.concatenate([part[:, hh * 256:hh * 256 + 128], part[:, hh * 256 + 128:hh * 256 + 256]], axis=0)
                qt[units[n], :, hh * 128:(hh + 1) * 128] = norm_rope(two.T, gq[...], cos, sin)

    def prologue(wk, wv, kst, vst, kf, vf):
        def cache_copy(src, dst, j, n):
            at = pl.ds(pl.multiple_of(j * CHUNK * KV, CHUNK * KV), CHUNK * KV)
            return pltpu.make_async_copy(src.at[at], dst.at[at], cache_sem.at[n, j])

        wk_copy = pltpu.make_async_copy(wk_hbm, wk, kv_sem.at[0])
        wv_copy = pltpu.make_async_copy(wv_hbm, wv, kv_sem.at[1])
        for j in range(EARLY):
            cache_copy(k_hbm, kst, j, 0).start()
            cache_copy(v_hbm, vst, j, 1).start()

        barrier = pltpu.get_barrier_semaphore()
        for to in (partner, cross):
            pl.semaphore_signal(barrier, inc=1, device_id=(dp, to), device_id_type=MESH)
        pl.semaphore_wait(barrier, 2)
        x_copy.wait()
        x_to_cross.start()
        x_to_partner.start()
        for c in small:
            c.start()
        for j in range(EARLY, GROUPS):
            cache_copy(k_hbm, kst, j, 0).start()
            cache_copy(v_hbm, vst, j, 1).start()
        wk_copy.start()
        wv_copy.start()
        for g in range(2):
            wq_copy(g).start()
        for m in range(1, 4):
            wq_copy(2 * m + core).start()
        for m in range(1, 4):
            wo_copy(2 * m + 1 - core).start()

        def relayout(j, carry):
            cache_copy(k_hbm, kst, j, 0).wait()
            cache_copy(v_hbm, vst, j, 1).wait()
            at = pl.ds(pl.multiple_of(j * CHUNK * KV, CHUNK * KV), CHUNK * KV)
            to = pl.ds(pl.multiple_of(j * CHUNK, CHUNK), CHUNK)
            kf[...] = kst[at].astype(F32)
            vf[...] = vst[at].astype(F32)
            for h in range(KV):
                ks[h, to, :] = kf[pl.ds(h, CHUNK, stride=KV), :].astype(BF16)
                vt[h, :, to] = vf[pl.ds(h, CHUNK, stride=KV), :].astype(BF16).T
            return carry

        lax.fori_loop(0, GROUPS, relayout, 0)

        for c in small:
            c.wait()
        gq[...] = jnp.broadcast_to(qg_ref[...].astype(F32), (HEAD_DIM, HEAD_DIM)).T
        gk[...] = jnp.broadcast_to(kg_ref[...].astype(F32), (HEAD_DIM, HEAD_DIM)).T
        normalise(0)
        x_to_partner.wait_recv()
        normalise(1)

        wk_copy.wait()
        wv_copy.wait()
        k_raw = jnp.dot(hbuf[0:ROWS, :], wk[...], preferred_element_type=F32).astype(BF16)
        v_raw = jnp.dot(hbuf[0:ROWS, :], wv[...], preferred_element_type=F32).astype(BF16)
        for hh in range(2):
            two = jnp.concatenate([k_raw[:, hh * 256:hh * 256 + 128], k_raw[:, hh * 256 + 128:hh * 256 + 256]], axis=0)
            back = norm_rope(two.T, gk[...], cos_ref[me], sin_ref[me]).T
            for n in range(2):
                ks[2 * hh + n, KEYS:ALL_KEYS, :] = back[n * ROWS:(n + 1) * ROWS]
                knew_ref[:, 2 * hh + n, :] = back[n * ROWS:(n + 1) * ROWS]
        for h in range(KV):
            one = v_raw[:, h * 128:(h + 1) * 128]
            vt[h, :, KEYS:ALL_KEYS] = one.T
            vnew_ref[:, h, :] = one

    def main(s_a, s_b):
        for g in range(2):
            wq_copy(g).wait()
            project(g)

        tiles = [(t * TILE, TILE) for t in range(KEYS // TILE)] + [(KEYS, ROWS)]

        def colmax(s, n):
            return jnp.max(s.reshape(n // 8, 8, COLS), axis=0)

        class Unit:
            pass

        def begin(u, s_ref, m_ref, dest):
            z = Unit()
            z.s, z.m = s_ref, m_ref
            z.peak = m_ref[0:1]
            z.head = place(u // 2)[0] // 2
            z.acc = z.sum = None
            return z

        def begin_next(z, u, s_ref, m_ref, dest):
            z.s, z.m = s_ref, m_ref
            z.next_head = place(u // 2)[0] // 2
            z.q = qt[u]
            z.dest = dest
            z.top = None
            return z

        def weigh(z, t):
            lo, n = tiles[t]
            p = jnp.exp2(z.s[lo:lo + n, :] * SCALE2 - z.peak)
            part = jnp.sum(p.reshape(n // 8, 8, COLS), axis=0)
            z.sum = part if z.sum is None else z.sum + part
            a = jnp.dot(vt[z.head, :, lo:lo + n], p.astype(BF16), preferred_element_type=F32)
            z.acc = a if z.acc is None else z.acc + a

        def score(z, t):
            lo, n = tiles[t]
            s = jnp.dot(ks[z.next_head, lo:lo + n, :], z.q, preferred_element_type=F32)
            if t == len(tiles) - 1:
                key = me * ROWS + lax.broadcasted_iota(jnp.int32, (n, COLS), 0)
                row = z.dest * ROWS + (lax.broadcasted_iota(jnp.int32, (n, COLS), 1) & (ROWS - 1))
                s = jnp.where(key <= row, s, -jnp.inf)
            z.s[lo:lo + n, :] = s
            top = colmax(s, n)
            z.top = top if z.top is None else jnp.maximum(z.top, top)

        def end_next(z):
            z.m[0:1] = jnp.max(z.top, axis=0, keepdims=True) * SCALE2

        def finish(z, ref, slot):
            ref[slot, 0:HEAD_DIM, :] = z.acc
            ref[slot, HEAD_DIM:HEAD_DIM + 1, :] = z.peak
            ref[slot, HEAD_DIM + 1:HEAD_DIM + 2, :] = jnp.sum(z.sum, axis=0, keepdims=True)

        def dests(i):
            own = place(i)[1]
            return jnp.where(own, partner, far), jnp.where(own, me, cross)

        za, zb = Unit(), Unit()
        da, db = partner, me
        begin_next(za, 0, s_a, m_a, da)
        begin_next(zb, 1, s_b, m_b, db)
        for t in range(len(tiles)):
            score(za, t)
            score(zb, t)
        end_next(za)
        end_next(zb)

        def to_partner(i):
            return remote(abuf.at[i], rbuf.at[i], as_sem.at[i], ar_sem.at[i], partner)

        def to_cross(g):
            return remote(bbuf.at[g + 2], cbuf.at[g], cs_sem.at[g], cr_sem.at[g], cross)

        def combine_cross(g):
            n = g + 2
            m1, m2 = bbuf[n, 128:129, :], rbuf[n, 128:129, :]
            m = jnp.maximum(m1, m2)
            w1, w2 = jnp.exp2(m1 - m), jnp.exp2(m2 - m)
            bbuf[n, 0:128, :] = bbuf[n, 0:128, :] * w1 + rbuf[n, 0:128, :] * w2
            total = bbuf[n, 129:130, :] * w1 + rbuf[n, 129:130, :] * w2
            bbuf[n, 128:129, :] = m
            bbuf[n, 129:130, :] = total

        def shared_place(m, c):
            return 4 + 2 * m + c

        def share(m, c):
            p = shared_place(m, c)
            return [remote(qt.at[2 * p + n], qt.at[2 * p + 1 - n], qs_sem.at[m, n], qr_sem.at[m, n], partner)
                    for n in range(2)]

        def attend(i, last, ahead=(), beside=None):
            a = begin(2 * i, s_a, m_a, None)
            b = begin(2 * i + 1, s_b, m_b, None)
            if not last:
                da, db = dests(i + 1)
                begin_next(a, 2 * i + 2, s_a, m_a, da)
                begin_next(b, 2 * i + 3, s_b, m_b, db)
            for t in range(len(tiles)):
                for z in (a, b):
                    weigh(z, t)
                    if not last:
                        score(z, t)
                for n, p in enumerate(ahead):
                    if t == 2 + 5 * n:
                        project(p)
                if beside is not None:
                    beside(t)
            finish(a, abuf, i)
            finish(b, bbuf, i)
            if not last:
                end_next(a)
                end_next(b)
            to_partner(i).start()

        def forward(t):
            if t == FORWARD_AT:
                x_to_cross.wait_recv()
                x_forward.start()

        def combining(i):
            to_partner(i - 2).wait_recv()

            def beside(t):
                if t == 1:
                    combine_cross(i - 4)

            return beside

        def pair(n, combine):
            i = 2 + 2 * n
            attend(i, False, beside=combining(i) if combine else None)
            if combine:
                to_cross(i - 4).start()
            beside = combining(i + 1) if combine else None
            for c in share(n, 1 - core):
                c.wait_recv()

            @pl.when(jnp.asarray(n) < 2)
            def _():
                wq_copy(2 * (n + 2) + core).wait()

            attend(i + 1, False, ahead=(shared_place(n + 1, core),), beside=beside)
            if combine:
                to_cross(i - 3).start()
            for c in share(n + 1, core):
                c.start()

            @pl.when(jnp.asarray(n) >= 2)
            def _():
                wo_copy(2 * (n - 1) + core).start()

        def body(n, carry):
            pair(n, True)
            return carry

        def late_body(i, carry):
            @pl.when(i == 2 * GROUPS - 3)
            def _():
                for c in share(SHARED - 1, 1 - core):
                    c.wait_recv()

            attend(i, False)
            return carry

        attend(0, False, beside=forward)
        normalise(2)
        x_forward.wait_recv()
        normalise(3)
        project(2)
        wq_copy(2 + core).wait()
        attend(1, False, ahead=(3, shared_place(0, core)))
        for c in share(0, core):
            c.start()
        wo_copy(0).start()
        wo_copy(1).start()
        pair(0, False)
        lax.fori_loop(1, 5, body, 0)
        lax.fori_loop(12, 15, late_body, 0)

        def slot_of(g):
            return g if g < 2 else GROUPS + g

        def arrive(g):
            to_partner(slot_of(g)).wait_recv()
            to_cross(g).wait_recv()

        def finish_group(g):
            parts = ((bbuf, slot_of(g)), (rbuf, slot_of(g)), (cbuf, g))
            peaks = [ref[n, 128:129, :] for ref, n in parts]
            m = jnp.maximum(jnp.maximum(peaks[0], peaks[1]), peaks[2])
            ws = [jnp.exp2(p - m) for p in peaks]
            total = sum(ref[n, 129:130, :] * w for (ref, n), w in zip(parts, ws))
            inv = 1.0 / total
            o = sum(ref[n, 0:128, :] * (w * inv) for (ref, n), w in zip(parts, ws)).astype(BF16)
            for hh in range(2):
                rows = o[:, hh * 128:(hh + 1) * 128].T
                for n in range(2):
                    col = (4 * g + 2 * hh + n) * HEAD_DIM
                    obuf[:, col:col + HEAD_DIM] = rows[n * ROWS:(n + 1) * ROWS]

        split = EARLY_OUT * 512

        def project_early(nb):
            cols = slice(nb * 512, (nb + 1) * 512)
            acc = jnp.dot(obuf[:, 0:2048], wbuf[2 * nb], preferred_element_type=F32)
            acc = acc + jnp.dot(obuf[:, 2048:split], wbuf[2 * nb + 1, 0:split - 2048], preferred_element_type=F32)
            part_out[:, cols] = acc

        def beside(t):
            if t < EARLY_OUT:
                finish_group(t)
            elif t in (7, 9, 11, 13):
                project_early((t - 7) // 2)

        for g in range(EARLY_OUT):
            arrive(g)
        for b in range(GROUPS):
            wo_copy(b).wait()
        attend(2 * GROUPS - 1, True, beside=beside)
        for g in range(EARLY_OUT, GROUPS):
            arrive(g)
        for g in range(EARLY_OUT, GROUPS):
            finish_group(g)
        for nb in range(4):
            cols = slice(nb * 512, (nb + 1) * 512)
            acc = jnp.dot(obuf[:, split:4096], wbuf[2 * nb + 1, split - 2048:2048], preferred_element_type=F32)
            out_ref[:, cols] = (xall[0, :, cols].astype(F32) + (part_out[:, cols] + acc)).astype(BF16)

        x_to_partner.wait_send()
        x_to_cross.wait_send()
        x_forward.wait_send()
        for m in range(SHARED):
            for c in share(m, core):
                c.wait_send()

        def drain(i, carry):
            to_partner(i).wait_send()
            return carry

        lax.fori_loop(0, 2 * GROUPS, drain, 0)

        def drain_cross(g, carry):
            to_cross(g).wait_send()
            return carry

        lax.fori_loop(0, GROUPS, drain_cross, 0)

    pl.run_scoped(
        prologue,
        pltpu.VMEM((HIDDEN, 512), BF16),
        pltpu.VMEM((HIDDEN, 512), BF16),
        pltpu.VMEM((KEYS * KV, HEAD_DIM), BF16),
        pltpu.VMEM((KEYS * KV, HEAD_DIM), BF16),
        pltpu.VMEM((CHUNK * KV, HEAD_DIM), F32),
        pltpu.VMEM((CHUNK * KV, HEAD_DIM), F32),
    )
    pl.run_scoped(main, pltpu.VMEM((ALL_KEYS, COLS), F32), pltpu.VMEM((ALL_KEYS, COLS), F32))

def hand_over(*refs):
    for src, dst in zip(refs[:3], refs[3:]):
        dst[...] = src[...]


def solution(mesh):
    row_spec = P(('dp', 'cp'), None)
    cache_spec = P(('dp', 'cp'), None, None)
    whole = P()
    any_spec = pl.BlockSpec(memory_space=pl.ANY)
    vmem_spec = pl.BlockSpec(memory_space=pltpu.VMEM)

    def device_step(x_rows, k_cache, v_cache, ln_gain, w_q, w_k, w_v, w_o, q_gain, k_gain):
        cos, sin = rope_tables(k_cache.shape[0] * CP)
        dma = pltpu.SemaphoreType.DMA
        results = pl.pallas_call(
            kernel,
            out_shape=(pltpu.VMEM((ROWS, HIDDEN), BF16),
                       pltpu.VMEM((ROWS, KV, HEAD_DIM), BF16),
                       pltpu.VMEM((ROWS, KV, HEAD_DIM), BF16)),
            in_specs=[any_spec] * 12,
            out_specs=(vmem_spec, vmem_spec, vmem_spec),
            scratch_shapes=[
                pltpu.VMEM((HIDDEN,), BF16),
                pltpu.VMEM((1, HEAD_DIM), BF16),
                pltpu.VMEM((1, HEAD_DIM), BF16),
                pltpu.VMEM((CP, HALF, 128), F32),
                pltpu.VMEM((CP, HALF, 128), F32),
                pltpu.VMEM((4, ROWS, HIDDEN), BF16),
                pltpu.VMEM((4 * ROWS, HIDDEN), BF16),
                pltpu.VMEM((GROUPS, 2048, 512), BF16),
                pltpu.VMEM((KV, ALL_KEYS, HEAD_DIM), BF16),
                pltpu.VMEM((KV, HEAD_DIM, ALL_KEYS), BF16),
                pltpu.VMEM((4 * GROUPS, HEAD_DIM, COLS), BF16),
                pltpu.VMEM((HEAD_DIM, HEAD_DIM), F32),
                pltpu.VMEM((HEAD_DIM, HEAD_DIM), F32),
                pltpu.VMEM((8, COLS), F32),
                pltpu.VMEM((8, COLS), F32),
                pltpu.VMEM((2 * GROUPS, MSG, COLS), F32),
                pltpu.VMEM((2 * GROUPS, MSG, COLS), F32),
                pltpu.VMEM((2 * GROUPS, MSG, COLS), F32),
                pltpu.VMEM((GROUPS, MSG, COLS), F32),
                pltpu.VMEM((ROWS, 4096), BF16),
                pltpu.VMEM((ROWS, HIDDEN), F32),
                dma, dma((3,)), dma((3,)), dma((GROUPS,)), dma((2,)), dma((5,)), dma((2, GROUPS)), dma((GROUPS,)),
                dma((2 * GROUPS,)), dma((2 * GROUPS,)), dma((GROUPS,)), dma((GROUPS,)),
                dma((SHARED, 2)), dma((SHARED, 2)),
            ],
            compiler_params=pltpu.CompilerParams(collective_id=0, has_side_effects=True,
                                                 vmem_limit_bytes=VMEM_LIMIT),
        )(x_rows, k_cache.reshape(-1, HEAD_DIM), v_cache.reshape(-1, HEAD_DIM), ln_gain, w_q, w_k, w_v, w_o,
          q_gain.reshape(1, -1), k_gain.reshape(1, -1), jnp.asarray(cos), jnp.asarray(sin))
        return pl.pallas_call(
            hand_over, out_shape=tuple(jax.ShapeDtypeStruct(r.shape, r.dtype) for r in results),
            in_specs=[vmem_spec] * 3, out_specs=(vmem_spec,) * 3,
        )(*[pltpu.with_memory_space_constraint(r, pltpu.VMEM) for r in results])

    return jax.shard_map(device_step, mesh=mesh,
                         in_specs=(row_spec, cache_spec, cache_spec, whole, whole, whole, whole, whole, whole, whole),
                         out_specs=(row_spec, cache_spec, cache_spec), check_vma=False)
```
